256 devices in a mesh: rep: 32 (over x_hi, z, core), tp: 8 (over x_lo, y).
Axes of the slice: x: 4 (x_hi: 2, x_lo: 2; x = x_hi * 2 + x_lo), y: 4, z: 8, core: 2. Of those that a mesh axis runs over, the one named last changes fastest.
Arguments:
- tokens: bfloat16 [32, 1024, 3072], P('rep', 'tp'), may hold values from -100 to 100
- norm_gain: float32 [32, 3072], P('rep'), may hold values from 0.5 to 1.5
- w_query: bfloat16 [32, 3072, 2048], P('rep', None, 'tp'), may hold values from -1 to 1
- key_weight: bfloat16 [32, 3072, 1024], P('rep', None, 'tp'), may hold values from -1 to 1
- value_weight: bfloat16 [32, 3072, 1024], P('rep', None, 'tp'), may hold values from -0.109375 to 0.109375
- attention_gradient: bfloat16 [32, 1024, 2048], P('rep', None, 'tp'), may hold values from -6 to 6
- global_fragment: float32 [512, 3072], P('tp'), may hold values from -6 to 6
- momentum: float32 [512, 3072], P('tp'), may hold values from -3 to 3
- local_fragment: bfloat16 [32, 512, 3072], P('rep', 'tp'), may hold values from -6 to 6
Outputs:
- grad_query_w: bfloat16 [32, 3072, 2048], P('rep', None, 'tp')
- grad_key_w: bfloat16 [32, 3072, 1024], P('rep', None, 'tp')
- grad_value_w: bfloat16 [32, 3072, 1024], P('rep', None, 'tp')
- grad_gain: float32 [32, 3072], P('rep')
- grad_tokens: bfloat16 [32, 1024, 3072], P('rep', 'tp')
- new_global: float32 [512, 3072], P('tp')
- new_momentum: float32 [512, 3072], P('tp')
The draws below stay inside these ranges and needn't reach their ends.
All inputs are finite; a program needn't handle non-finite values.
Results may differ from the reference program's by a relative error of at most 0.019.
The reference program's roundings to bfloat16 on the way count: a program that leaves them out, or rounds other values in their place, can miss the bound.
Values may be sent and summed in bfloat16 or wider, within the bound.
A program may use at most 128 MiB of HBM per device.

```python
import math
import jax
import jax.numpy as jnp
from jax import lax

MODEL_WIDTH = 3072
QUERY_HEADS = 16
KEY_VALUE_HEADS = 8
HEAD_SIZE = 128
SEQ = 1024
FRAG = 512
N_REP = 32
N_TP = 8


def draw_tokens(key, part):
    col_scale = jnp.exp(jax.random.uniform(jax.random.fold_in(key, 12), (1, 1, MODEL_WIDTH), jnp.float32, math.log(0.5), math.log(2.0)))
    row_scale = jnp.exp(jax.random.uniform(jax.random.fold_in(key, 11), (N_REP, SEQ, 1), jnp.float32, 0.0, math.log(10.0)))
    jitter = jax.random.normal(jax.random.fold_in(key, 13), (N_REP, SEQ, MODEL_WIDTH), jnp.float32)
    result = jitter * col_scale * row_scale
    return jnp.clip(result, -100.0, 100.0).astype(jnp.bfloat16)


def draw_w_query(key, part):
    return (jax.random.normal(jax.random.fold_in(key, 21), (N_REP, MODEL_WIDTH, QUERY_HEADS * HEAD_SIZE), jnp.float32) * MODEL_WIDTH ** (-0.5)).astype(jnp.bfloat16)


def draw_key_weight(key, part):
    return (jax.random.normal(jax.random.fold_in(key, 31), (N_REP, MODEL_WIDTH, KEY_VALUE_HEADS * HEAD_SIZE), jnp.float32) * MODEL_WIDTH ** (-0.5)).astype(jnp.bfloat16)


def levels(own_key, shape, pieces, low, largest):
    level, own = 1.0, jax.random.fold_in(own_key, 6)
    for dim, parts in pieces:
        heights = jnp.exp(jax.random.uniform(jax.random.fold_in(own, dim), (parts,), jnp.float32, low / len(pieces), largest / len(pieces)))
        level = level * jnp.repeat(heights, shape[dim] // parts).reshape([-1 if axis == dim else 1 for axis in range(len(shape))])
    return level


def centred(own_key, shape, spread, reach, cuts=(), kind=jnp.bfloat16):
    array = jax.random.normal(own_key, shape, jnp.float32) * spread
    if len(cuts) > 0:
        array = levels(own_key, shape, cuts, -0.22, 0.18) * array
    return jnp.clip(array, min=-reach, max=reach).astype(kind)


def setup_inputs(seed: int = 0) -> dict:
    seeds = jax.random.split(jax.random.key(seed), 10)
    return {
        "tokens": draw_tokens(jax.random.fold_in(seeds[9], 71), 0),
        "norm_gain": jnp.clip(1.0 + 0.1 * jax.random.normal(seeds[1], (N_REP, MODEL_WIDTH), jnp.float32), 0.5, 1.5),
        "w_query": draw_w_query(jax.random.fold_in(seeds[9], 71), 0),
        "key_weight": draw_key_weight(jax.random.fold_in(seeds[9], 71), 0),
        "value_weight": centred(seeds[4], (N_REP, MODEL_WIDTH, KEY_VALUE_HEADS * HEAD_SIZE), MODEL_WIDTH ** -0.5, 0.109375, ((0, 32), (2, 8))),
        "attention_gradient": centred(seeds[5], (N_REP, SEQ, QUERY_HEADS * HEAD_SIZE), 1.0, 6.0, ((0, 32), (2, 8))),
        "global_fragment": centred(seeds[6], (FRAG, MODEL_WIDTH), 1.0, 6.0, ((0, 8),), jnp.float32),
        "momentum": centred(seeds[7], (FRAG, MODEL_WIDTH), 0.5, 3.0, ((0, 8),), jnp.float32),
        "local_fragment": centred(seeds[8], (N_REP, FRAG, MODEL_WIDTH), 1.0, 6.0, ((0, 32), (1, 8))),
    }


epsilon = 1e-05
rope_base = 500000.0
outer_rate = 0.7
outer_momentum = 0.9

def rope_tables(sequence_length, width):
    middle = width // 2
    frequency = rope_base ** (-2.0 * jnp.arange(middle, dtype=jnp.float32) / width)
    angles = jnp.arange(sequence_length, dtype=jnp.float32)[:, None] * frequency[None, :]
    angles = jnp.concatenate([angles, angles], axis=1)
    return (jnp.cos(angles)[:, None, :], jnp.sin(angles)[:, None, :])

def rotate(vectors, cosine_table, sine_table):
    middle = vectors.shape[-1] // 2
    turned = jnp.concatenate([-vectors[..., middle:], vectors[..., :middle]], axis=-1)
    return vectors * cosine_table + turned * sine_table

def reverse_rotation(gradient, cosine_table, sine_table):
    middle = gradient.shape[-1] // 2
    shifted = gradient * sine_table
    turned = jnp.concatenate([shifted[..., middle:], -shifted[..., :middle]], axis=-1)
    return gradient * cosine_table + turned

def attention_reverse(query_rows, rotated_keys, values_bfloat, grad_out, block_of_rows):
    sequence_length = query_rows.shape[0]
    score_scale = query_rows.shape[-1] ** (-0.5)
    keys_wide = rotated_keys.astype(jnp.float32)
    values_wide = values_bfloat.astype(jnp.float32)

    def one_block(running, block_index):
        acc_key, acc_value = running
        offset = block_index * block_of_rows
        query_block = lax.dynamic_slice_in_dim(query_rows, offset, block_of_rows, 0).astype(jnp.float32)
        grad_block = lax.dynamic_slice_in_dim(grad_out, offset, block_of_rows, 0).astype(jnp.float32)
        scores = jnp.einsum('qgrd,kgd->grqk', query_block, keys_wide) * score_scale
        row_pos = offset + jnp.arange(block_of_rows)
        col_pos = jnp.arange(sequence_length)
        allowed = col_pos[None, :] <= row_pos[:, None]
        scores = jnp.where(allowed, scores, -jnp.inf)
        highest = lax.optimization_barrier(jnp.max(scores, axis=-1, keepdims=True))
        powers = jnp.exp(scores - highest)
        probability = powers / lax.optimization_barrier(jnp.sum(powers, axis=-1, keepdims=True))
        prob_low = lax.optimization_barrier(probability.astype(jnp.bfloat16)).astype(jnp.float32)
        acc_value = acc_value + jnp.einsum('grqk,qgrd->kgd', prob_low, grad_block)
        grad_prob = jnp.einsum('qgrd,kgd->grqk', grad_block, values_wide)
        grad_score = probability * (grad_prob - lax.optimization_barrier(jnp.sum(grad_prob * probability, axis=-1, keepdims=True))) * score_scale
        score_low = lax.optimization_barrier(grad_score.astype(jnp.bfloat16)).astype(jnp.float32)
        grad_query = jnp.einsum('grqk,kgd->qgrd', score_low, keys_wide)
        acc_key = acc_key + jnp.einsum('grqk,qgrd->kgd', score_low, query_block)
        return ((acc_key, acc_value), grad_query)
    initial = jnp.zeros(rotated_keys.shape, jnp.float32)
    (acc_key, acc_value), grad_blocks = lax.scan(one_block, (initial, initial), jnp.arange(sequence_length // block_of_rows))
    grad_query = grad_blocks.reshape(query_rows.shape)
    return (grad_query, acc_key, acc_value)

def replica_grads(items):
    tokens, norm_gains, w_query, key_weight, value_weight, attention_gradient = items
    sequence_length = tokens.shape[0]
    widened_rows = tokens.astype(jnp.float32)
    inverse_norm = lax.rsqrt(lax.optimization_barrier(jnp.mean(widened_rows * widened_rows, axis=-1, keepdims=True)) + epsilon)
    normalized_input = widened_rows * inverse_norm
    normalized = (normalized_input * norm_gains[None, :]).astype(jnp.bfloat16)
    cosine_table, sine_table = rope_tables(sequence_length, HEAD_SIZE)
    query_rows = jnp.dot(normalized, w_query, preferred_element_type=jnp.float32).reshape(sequence_length, QUERY_HEADS, HEAD_SIZE)
    query_rows = rotate(query_rows, cosine_table, sine_table).astype(jnp.bfloat16)
    rotated_keys = jnp.dot(normalized, key_weight, preferred_element_type=jnp.float32).reshape(sequence_length, KEY_VALUE_HEADS, HEAD_SIZE)
    rotated_keys = rotate(rotated_keys, cosine_table, sine_table).astype(jnp.bfloat16)
    values_bfloat = jnp.dot(normalized, value_weight, preferred_element_type=jnp.float32).astype(jnp.bfloat16).reshape(sequence_length, KEY_VALUE_HEADS, HEAD_SIZE)
    replica_group = QUERY_HEADS // KEY_VALUE_HEADS
    block_of_rows = min(512, sequence_length)
    query_input_gradient, key_input_gradient, value_input_gradient = attention_reverse(query_rows.reshape(sequence_length, KEY_VALUE_HEADS, replica_group, HEAD_SIZE), rotated_keys, values_bfloat, attention_gradient.reshape(sequence_length, KEY_VALUE_HEADS, replica_group, HEAD_SIZE), block_of_rows)
    dquery = reverse_rotation(query_input_gradient.reshape(sequence_length, QUERY_HEADS, HEAD_SIZE), cosine_table, sine_table).astype(jnp.bfloat16).reshape(sequence_length, QUERY_HEADS * HEAD_SIZE)
    key_gradient = reverse_rotation(key_input_gradient, cosine_table, sine_table).astype(jnp.bfloat16).reshape(sequence_length, KEY_VALUE_HEADS * HEAD_SIZE)
    value_gradient = value_input_gradient.astype(jnp.bfloat16).reshape(sequence_length, KEY_VALUE_HEADS * HEAD_SIZE)
    contract = (((0,), (0,)), ((), ()))
    grad_wq = lax.dot_general(normalized, dquery, contract, preferred_element_type=jnp.float32).astype(jnp.bfloat16)
    grad_wk = lax.dot_general(normalized, key_gradient, contract, preferred_element_type=jnp.float32).astype(jnp.bfloat16)
    grad_wv = lax.dot_general(normalized, value_gradient, contract, preferred_element_type=jnp.float32).astype(jnp.bfloat16)
    query_cols = QUERY_HEADS * HEAD_SIZE // N_TP
    key_value_columns = KEY_VALUE_HEADS * HEAD_SIZE // N_TP
    back = (((1,), (1,)), ((), ()))
    summed_rows = jnp.zeros((sequence_length, MODEL_WIDTH), jnp.float32)
    for shard_index in range(N_TP):
        qa, qb_end = (shard_index * query_cols, (shard_index + 1) * query_cols)
        ka, kb_end = (shard_index * key_value_columns, (shard_index + 1) * key_value_columns)
        partial_value = lax.dot_general(dquery[:, qa:qb_end], w_query[:, qa:qb_end], back, preferred_element_type=jnp.float32)
        partial_value = partial_value + lax.dot_general(key_gradient[:, ka:kb_end], key_weight[:, ka:kb_end], back, preferred_element_type=jnp.float32)
        partial_value = partial_value + lax.dot_general(value_gradient[:, ka:kb_end], value_weight[:, ka:kb_end], back, preferred_element_type=jnp.float32)
        summed_rows = summed_rows + lax.optimization_barrier(partial_value.astype(jnp.bfloat16)).astype(jnp.float32)
    gains_gradient = lax.optimization_barrier(jnp.sum(summed_rows * normalized_input, axis=0))
    scaled_rows = summed_rows * norm_gains[None, :]
    gradient_rows = inverse_norm * (scaled_rows - normalized_input * lax.optimization_barrier(jnp.mean(scaled_rows * normalized_input, axis=-1, keepdims=True)))
    return (grad_wq, grad_wk, grad_wv, gains_gradient, gradient_rows.astype(jnp.bfloat16))

def reference(tokens, norm_gain, w_query, key_weight, value_weight, attention_gradient, global_fragment, momentum, local_fragment):
    grad_wq, grad_wk, grad_wv, gains_gradient, gradient_rows = lax.map(replica_grads, (tokens, norm_gain, w_query, key_weight, value_weight, attention_gradient))
    delta = global_fragment[None, :, :] - local_fragment.astype(jnp.float32)
    mean_delta = lax.optimization_barrier(jnp.sum(delta, axis=0)) / N_REP
    new_momentum = outer_momentum * momentum + mean_delta
    new_global = global_fragment - outer_rate * (mean_delta + outer_momentum * new_momentum)
    return (grad_wq, grad_wk, grad_wv, gains_gradient, gradient_rows, new_global, new_momentum)
```

```python
import jax
import jax.numpy as jnp
import numpy as np
from jax import lax
from jax.experimental import pallas as pl
from jax.experimental.pallas import tpu as pltpu
from jax.sharding import PartitionSpec as P

HEAD = 128
EPSILON = 1e-05
ROPE_BASE = 500000.0
OUTER_RATE = 0.7
OUTER_MOMENTUM = 0.9
NEGATIVE = -1e30


def rope_constants(seq):
    half = HEAD // 2
    freq = ROPE_BASE ** (-2.0 * np.arange(half, dtype=np.float64) / HEAD)
    angle = np.arange(seq, dtype=np.float64)[:, None] * freq[None, :]
    cos, sin = np.cos(angle), np.sin(angle)
    table = np.concatenate([cos, cos, -sin, sin], axis=1)
    return jnp.asarray(table.astype(np.float32))


def rope(v, cos, sin):
    return v * cos + pltpu.roll(v, HEAD // 2, 1) * sin


def unrope(g, cos, sin):
    return g * cos - pltpu.roll(g, HEAD // 2, 1) * sin


def project(rows, x, weights, table, qkv):
    heads = qkv.shape[1] // HEAD
    cos = table[rows, :HEAD]
    sin = table[rows, HEAD:]
    out = jnp.dot(x, weights[...], preferred_element_type=jnp.float32)
    for h in range(heads):
        part = out[:, h * HEAD : (h + 1) * HEAD]
        if h < heads - 1:
            part = rope(part, cos, sin)
        qkv[rows, h * HEAD : (h + 1) * HEAD] = part.astype(jnp.bfloat16)


def dot_t(a, b):
    return lax.dot_general(a, b, (((1,), (1,)), ((), ())), preferred_element_type=jnp.float32)


def t_dot(a, b):
    return lax.dot_general(a, b, (((0,), (0,)), ((), ())), preferred_element_type=jnp.float32)


def attention_rows(start, block, qkv, dout, table, dqkv, acc_k, acc_v, first):
    width = start + block
    scale = HEAD ** (-0.5)
    heads = dout.shape[1] // HEAD
    at_k, at_v = heads * HEAD, (heads + 1) * HEAD
    keys = qkv[:width, at_k : at_k + HEAD]
    values = qkv[:width, at_v : at_v + HEAD]
    rows = slice(start, start + block)
    row = lax.broadcasted_iota(jnp.int32, (block, block), 0)
    col = lax.broadcasted_iota(jnp.int32, (block, block), 1)
    allowed = col <= row
    cos, sin = table[rows, :HEAD], table[rows, HEAD:]
    dk = dv = None
    for h in range(heads):
        q = qkv[rows, h * HEAD : (h + 1) * HEAD]
        do = dout[rows, h * HEAD : (h + 1) * HEAD]
        s = dot_t(q, keys)
        last = jnp.where(allowed, s[:, start:], NEGATIVE)
        s = last if start == 0 else jnp.concatenate([s[:, :start], last], axis=1)
        top = jnp.max(s, axis=1, keepdims=True)
        power = jnp.exp((s - top) * scale)
        p = power * (1.0 / jnp.sum(power, axis=1, keepdims=True))
        dp = dot_t(do, values)
        drop = jnp.sum(dp * p, axis=1, keepdims=True)
        ds = ((p * (dp - drop)) * scale).astype(jnp.bfloat16)
        p_low = p.astype(jnp.bfloat16)
        dq = jnp.dot(ds, keys, preferred_element_type=jnp.float32)
        dqkv[rows, h * HEAD : (h + 1) * HEAD] = unrope(dq, cos, sin).astype(jnp.bfloat16)
        tv, tk = t_dot(p_low, do), t_dot(ds, q)
        dv = tv if dv is None else dv + tv
        dk = tk if dk is None else dk + tk
    if first:
        acc_v[:width, :] = dv
        acc_k[:width, :] = dk
    else:
        acc_v[:width, :] += dv
        acc_k[:width, :] += dk
    width = start
    heads_at = heads * HEAD
    dqkv[rows, heads_at : heads_at + HEAD] = unrope(acc_k[rows, :], cos, sin).astype(jnp.bfloat16)
    dqkv[rows, heads_at + HEAD : heads_at + 2 * HEAD] = acc_v[rows, :].astype(jnp.bfloat16)


def attention(block, qkv, dout, table, dqkv, acc_k, acc_v):
    seq = qkv.shape[0]
    for start in reversed(range(0, seq, block)):
        attention_rows(start, block, qkv, dout, table, dqkv, acc_k, acc_v, start + block == seq)


def weight_grads(x, dqkv, block, outs):
    depth = x.shape[1]

    def one(j, carry):
        at = pl.multiple_of(j * block, block)
        g = t_dot(x[:, pl.ds(at, block)], dqkv[...]).astype(jnp.bfloat16)
        done = 0
        for o in outs:
            o[pl.ds(at, block), :] = g[:, done : done + o.shape[1]]
            done += o.shape[1]
        return carry

    lax.fori_loop(0, depth // block, one, 0)


def local_kernel(x, wq, wk, wv, dout, table, part, gq, gk, gv, weights, qkv, dqkv, acc_k, acc_v):
    seq, depth = x.shape
    weights[:, : wq.shape[1]] = wq[...]
    weights[:, wq.shape[1] : wq.shape[1] + HEAD] = wk[...]
    weights[:, wq.shape[1] + HEAD :] = wv[...]
    rows = 256

    def proj(i, carry):
        r = pl.ds(pl.multiple_of(i * rows, rows), rows)
        project(r, x[r, :], weights, table, qkv)
        return carry

    lax.fori_loop(0, seq // rows, proj, 0)
    attention(256, qkv, dout, table, dqkv, acc_k, acc_v)

    def back(i, carry):
        r = pl.ds(pl.multiple_of(i * rows, rows), rows)
        part[r, :] = dot_t(dqkv[r, :], weights[...]).astype(jnp.bfloat16)
        return carry

    lax.fori_loop(0, seq // rows, back, 0)
    weight_grads(x, dqkv, 256, (gq, gk, gv))


def local(x, wq, wk, wv, dout):
    seq, depth = x.shape
    table = rope_constants(seq)
    bf = jnp.bfloat16
    cols = wq.shape[1] + wk.shape[1] + wv.shape[1]
    vm = pl.BlockSpec(memory_space=pltpu.VMEM)
    return pl.pallas_call(
        local_kernel,
        out_shape=(
            jax.ShapeDtypeStruct((seq, depth), bf),
            jax.ShapeDtypeStruct(wq.shape, bf),
            jax.ShapeDtypeStruct(wk.shape, bf),
            jax.ShapeDtypeStruct(wv.shape, bf),
        ),
        in_specs=[vm] * 6,
        out_specs=[vm] * 4,
        scratch_shapes=[
            pltpu.VMEM((depth, cols), bf),
            pltpu.VMEM((seq, cols), bf),
            pltpu.VMEM((seq, cols), bf),
            pltpu.VMEM((seq, HEAD), jnp.float32),
            pltpu.VMEM((seq, HEAD), jnp.float32),
        ],
        compiler_params=pltpu.CompilerParams(vmem_limit_bytes=60 * 1024 * 1024),
        cost_estimate=pl.CostEstimate(
            flops=2 * seq * cols * depth * 3, bytes_accessed=20_000_000, transcendentals=0
        ),
    )(x, wq, wk, wv, dout, table)


def body(tokens, norm_gain, w_query, key_weight, value_weight, attention_gradient, global_fragment, momentum, local_fragment):
    gain = norm_gain[0]
    wide = tokens[0].astype(jnp.float32)
    inverse = lax.rsqrt(jnp.mean(wide * wide, axis=-1, keepdims=True) + EPSILON)
    xhat = wide * inverse
    normed = lax.all_gather((xhat * gain[None, :]).astype(jnp.bfloat16), "tp", axis=0, tiled=True)
    part, gq, gk, gv = local(normed, w_query[0], key_weight[0], value_weight[0], attention_gradient[0])
    summed = lax.psum_scatter(part, "tp", scatter_dimension=0, tiled=True).astype(jnp.float32)
    own = jnp.sum(summed * xhat, axis=0)
    grad_gain = jnp.sum(lax.all_gather(own, "tp", axis=0), axis=0)
    scaled = summed * gain[None, :]
    grad_tokens = (inverse * (scaled - xhat * jnp.mean(scaled * xhat, axis=-1, keepdims=True))).astype(jnp.bfloat16)
    replicas = lax.axis_size("rep")
    rows = global_fragment.shape[0] // replicas
    mine = local_fragment[0].reshape(replicas, rows, -1)
    arrived = lax.all_to_all(mine, "rep", split_axis=0, concat_axis=0, tiled=True)
    at = lax.axis_index("rep") * rows
    globals_ = lax.dynamic_slice_in_dim(global_fragment, at, rows, 0)
    mean_rows = globals_ - jnp.sum(arrived.astype(jnp.float32), axis=0) / replicas
    mean = lax.all_gather(mean_rows, "rep", axis=0, tiled=True)
    new_momentum = OUTER_MOMENTUM * momentum + mean
    new_global = global_fragment - OUTER_RATE * (mean + OUTER_MOMENTUM * new_momentum)
    return (gq[None], gk[None], gv[None], grad_gain[None], grad_tokens[None], new_global, new_momentum)


def solution(mesh):
    placed = (
        P("rep", "tp", None), P("rep", None), P("rep", None, "tp"), P("rep", None, "tp"), P("rep", None, "tp"),
        P("rep", None, "tp"), P("tp", None), P("tp", None), P("rep", "tp", None),
    )
    outs = (P("rep", None, "tp"), P("rep", None, "tp"), P("rep", None, "tp"), P("rep", None), P("rep", "tp", None), P("tp", None), P("tp", None))
    return jax.shard_map(body, mesh=mesh, in_specs=placed, out_specs=outs, check_vma=False)
```

```python
import functools

import jax
import jax.numpy as jnp
import numpy as np
from jax import lax
from jax.experimental import pallas as pl
from jax.experimental.pallas import tpu as pltpu
from jax.sharding import PartitionSpec as P

HEAD = 128
EPSILON = 1e-05
ROPE_BASE = 500000.0
OUTER_RATE = 0.7
OUTER_MOMENTUM = 0.9
NEGATIVE = -1e30


def rope_constants(seq):
    half = HEAD // 2
    freq = ROPE_BASE ** (-2.0 * np.arange(half, dtype=np.float64) / HEAD)
    angle = np.arange(seq, dtype=np.float64)[:, None] * freq[None, :]
    cos, sin = np.cos(angle), np.sin(angle)
    table = np.concatenate([cos, cos, -sin, sin], axis=1)
    return jnp.asarray(table.astype(np.float32))


def rope(v, cos, sin):
    return v * cos + pltpu.roll(v, HEAD // 2, 1) * sin


def unrope(g, cos, sin):
    return g * cos - pltpu.roll(g, HEAD // 2, 1) * sin


def project(rows, x, weights, table, qkv):
    heads = qkv.shape[1] // HEAD
    cos = table[rows, :HEAD]
    sin = table[rows, HEAD:]
    out = jnp.dot(x, weights[...], preferred_element_type=jnp.float32)
    for h in range(heads):
        part = out[:, h * HEAD : (h + 1) * HEAD]
        if h < heads - 1:
            part = rope(part, cos, sin)
        qkv[rows, h * HEAD : (h + 1) * HEAD] = part.astype(jnp.bfloat16)


def dot_t(a, b):
    return lax.dot_general(a, b, (((1,), (1,)), ((), ())), preferred_element_type=jnp.float32)


def t_dot(a, b):
    return lax.dot_general(a, b, (((0,), (0,)), ((), ())), preferred_element_type=jnp.float32)


def attention_rows(start, block, qkv, dout, table, dqkv, acc_k, acc_v, first):
    width = start + block
    scale = HEAD ** (-0.5)
    heads = dout.shape[1] // HEAD
    at_k, at_v = heads * HEAD, (heads + 1) * HEAD
    keys = qkv[:width, at_k : at_k + HEAD]
    values = qkv[:width, at_v : at_v + HEAD]
    rows = slice(start, start + block)
    row = lax.broadcasted_iota(jnp.int32, (block, block), 0)
    col = lax.broadcasted_iota(jnp.int32, (block, block), 1)
    allowed = col <= row
    cos, sin = table[rows, :HEAD], table[rows, HEAD:]
    dk = dv = None
    for h in range(heads):
        q = qkv[rows, h * HEAD : (h + 1) * HEAD]
        do = dout[rows, h * HEAD : (h + 1) * HEAD]
        s = dot_t(q, keys)
        last = jnp.where(allowed, s[:, start:], NEGATIVE)
        s = last if start == 0 else jnp.concatenate([s[:, :start], last], axis=1)
        top = jnp.max(s, axis=1, keepdims=True)
        power = jnp.exp((s - top) * scale)
        p = power * (1.0 / jnp.sum(power, axis=1, keepdims=True))
        dp = dot_t(do, values)
        drop = jnp.sum(dp * p, axis=1, keepdims=True)
        ds = ((p * (dp - drop)) * scale).astype(jnp.bfloat16)
        p_low = p.astype(jnp.bfloat16)
        dq = jnp.dot(ds, keys, preferred_element_type=jnp.float32)
        dqkv[rows, h * HEAD : (h + 1) * HEAD] = unrope(dq, cos, sin).astype(jnp.bfloat16)
        tv, tk = t_dot(p_low, do), t_dot(ds, q)
        dv = tv if dv is None else dv + tv
        dk = tk if dk is None else dk + tk
    if first:
        acc_v[:width, :] = dv
        acc_k[:width, :] = dk
    else:
        acc_v[:width, :] += dv
        acc_k[:width, :] += dk
    width = start
    heads_at = heads * HEAD
    dqkv[rows, heads_at : heads_at + HEAD] = unrope(acc_k[rows, :], cos, sin).astype(jnp.bfloat16)
    dqkv[rows, heads_at + HEAD : heads_at + 2 * HEAD] = acc_v[rows, :].astype(jnp.bfloat16)


def attention(block, qkv, dout, table, dqkv, acc_k, acc_v):
    seq = qkv.shape[0]
    for start in reversed(range(0, seq, block)):
        attention_rows(start, block, qkv, dout, table, dqkv, acc_k, acc_v, start + block == seq)


ROWS = 128
UNIT = 16
UNITS = ROWS // UNIT
FIRST = 5
STEPS = 12


def units(count, step, start=0):
    def one(i, carry):
        step(i)
        return carry

    lax.fori_loop(start, start + count, one, 0)


def normalise(rows, tokens):
    wide = tokens[rows, :].astype(jnp.float32)
    inverse = lax.rsqrt(jnp.mean(wide * wide, axis=1, keepdims=True) + EPSILON)
    return wide * inverse, inverse


def step_kernel(
    reps,
    tokens_h, gain_h, wq_h, wk_h, wv_h, dout_h, table_h, global_h, local_h,
    gq_h, gk_h, gv_h, ggain_h, gtok_h, mean_h,
    tokens, gain, xf, weights, qkv, dqkv, dout, table, acc_k, acc_v,
    part, full_p, full_m, half_p, half_m, from_x,
    gq, gk, gv, gtok, gbuf, gsum, gfin,
    frag, buf_a, acc_a, buf_c, acc_c, buf_b, mean_a, mean_o, gpiece,
    load, store,
    asp, asm, asx, arp, arm, arx,
    rsp, rsm, rsx, rrp, rrm, rrx,
    gs, gr, fs, fr, fcs, fcr, fds, fdr,
):
    f32, bf = jnp.float32, jnp.bfloat16
    depth = xf.shape[1]
    mid = depth // 2
    r, t = lax.axis_index("rep"), lax.axis_index("tp")
    nz = reps // 4
    xh, z, core = r // (2 * nz), (r // 2) % nz, r % 2
    cx, y = t // 4, t % 4
    ox = 1 - cx
    up, dn, far = (y + 1) % 4, (y + 3) % 4, (y + 2) % 4

    def tp_dev(col, row):
        return (r, col * 4 + row)

    def rep_dev(h, zz, c):
        return (h * (2 * nz) + zz * 2 + c, t)

    dev_p, dev_m, dev_x = tp_dev(cx, up), tp_dev(cx, dn), tp_dev(ox, y)
    dev_core, dev_h = rep_dev(xh, z, 1 - core), rep_dev(1 - xh, z, core)

    def rdma(src, dst, s, d, dev):
        return pltpu.make_async_remote_copy(
            src_ref=src, dst_ref=dst, send_sem=s, recv_sem=d,
            device_id=dev, device_id_type=pl.DeviceIdType.MESH,
        )

    wide_q = wq_h.shape[1]
    loads = [
        (tokens_h, tokens),
        (gain_h, gain),
        (local_h, frag),
        (wq_h, weights.at[:, :wide_q]),
        (wk_h, weights.at[:, wide_q : wide_q + HEAD]),
        (wv_h, weights.at[:, wide_q + HEAD :]),
        (table_h, table),
        (dout_h, dout),
        (
            global_h.at[
                pl.ds(pl.multiple_of(core * 32 + xh * 16, 16), 16),
                pl.ds(pl.multiple_of(z * (depth // nz), 128), depth // nz),
            ],
            gpiece,
        ),
    ]
    loads = [pltpu.make_async_copy(a, b, load.at[i]) for i, (a, b) in enumerate(loads)]
    for c in loads:
        c.start()

    barrier = pltpu.get_barrier_semaphore()
    peers = [(r, (t + d) % 8) for d in range(1, 8)]
    peers += [dev_core, dev_h] + [rep_dev(xh, (z + d) % nz, core) for d in range(1, nz)]
    for p in peers:
        pl.semaphore_signal(barrier, inc=1, device_id=p, device_id_type=pl.DeviceIdType.MESH)
    loads[0].wait()
    loads[1].wait()
    loads[2].wait()
    pl.semaphore_wait(barrier, len(peers))

    def frag_a():
        other = pl.ds(pl.multiple_of((1 - core) * 32, 32), 32)
        return rdma(frag.at[other, :], buf_a, fs.at[0], fr.at[0], dev_core)

    frag_a().start()

    def place(ref, col, row, u, half=None):
        rows = pl.ds(pl.multiple_of((col * 4 + row) * ROWS + u * UNIT, UNIT), UNIT)
        if half is None:
            return ref.at[rows, :]
        return ref.at[rows, half * mid : (half + 1) * mid]

    def gather(way, i, col, row, u, half=None):
        s, d, dev = ((asp, arp, dev_p), (asm, arm, dev_m), (asx, arx, dev_x))[way]
        ref = place(xf, col, row, u, half)
        return rdma(ref, ref, s.at[i], d.at[i], dev)

    def norm_unit(i):
        u = (i + FIRST) % UNITS
        rows = pl.ds(pl.multiple_of(u * UNIT, UNIT), UNIT)
        xhat, _ = normalise(rows, tokens)
        at = pl.ds(pl.multiple_of(t * ROWS + u * UNIT, UNIT), UNIT)
        xf[at, :] = (xhat * gain[...]).astype(bf)

    def send_own(i):
        u = (i + FIRST) % UNITS
        for way in range(3):
            gather(way, u, cx, y, u).start()

    norm_unit(0)

    def norm_and_send(i):
        norm_unit(i)
        send_own(i - 1)

    units(UNITS - 1, norm_and_send, 1)
    for c in loads[3:]:
        c.wait()
    send_own(UNITS - 1)

    later = UNITS - FIRST

    def relay_later(i):
        u = FIRST + i
        gather(0, u, cx, dn, u).wait_recv()
        gather(0, 13 + u, cx, dn, u, 0).start()
        gather(2, 8 + i, cx, dn, u).start()
        gather(1, u, cx, up, u).wait_recv()
        gather(1, 13 + u, cx, up, u, 1).start()
        gather(2, 11 + i, cx, up, u).start()

    def relay_first(u):
        gather(0, u, cx, dn, u).wait_recv()
        gather(0, 13 + u, cx, dn, u, 0).start()
        gather(1, u, cx, up, u).wait_recv()
        gather(1, 13 + u, cx, up, u, 1).start()
        gather(2, u, ox, y, u).wait_recv()
        gather(0, 8 + u, ox, y, u).start()
        gather(1, 8 + u, ox, y, u).start()

    def relay_far(i):
        u = FIRST + i
        gather(0, 13 + u, cx, far, u, 0).wait_recv()
        gather(1, 13 + u, cx, far, u, 1).wait_recv()
        gather(2, 14 + i, cx, far, u).start()

    def relay_other(u):
        gather(0, 8 + u, ox, dn, u).wait_recv()
        gather(0, 21 + u, ox, dn, u, 0).start()
        gather(1, 8 + u, ox, up, u).wait_recv()
        gather(1, 21 + u, ox, up, u, 1).start()

    zcols = depth // nz

    def frag_c(d):
        peer = (z + d) % nz
        return rdma(
            acc_a.at[:, pl.ds(pl.multiple_of(peer * zcols, 128), zcols)], buf_c.at[z],
            fcs.at[d], fcr.at[d], rep_dev(xh, peer, core),
        )

    def frag_b():
        other = pl.ds(pl.multiple_of((1 - xh) * 16, 16), 16)
        return rdma(acc_c.at[other, :], buf_b, fs.at[1], fr.at[1], dev_h)

    def frag_b_back():
        mine = mean_a.at[z, pl.ds(pl.multiple_of(xh * 16, 16), 16), :]
        return rdma(mine, mine, fs.at[2], fr.at[2], dev_h)

    def frag_c_back(d):
        return rdma(mean_a.at[z], mean_a.at[z], fds.at[d], fdr.at[d], rep_dev(xh, (z + d) % nz, core))

    def frag_a_back():
        return rdma(mean_a, mean_o, fs.at[3], fr.at[3], dev_core)

    def frag_step(k):
        if k == 0:
            frag_a().wait_recv()
            own = frag[pl.ds(pl.multiple_of(core * 32, 32), 32), :]
            acc_a[...] = own.astype(f32) + buf_a[...].astype(f32)
        elif k == 1:
            for d in range(1, nz):
                frag_c(d).start()
        elif k == 2:
            for d in range(1, nz):
                frag_c(d).wait_recv()
            total = acc_a[:, pl.ds(pl.multiple_of(z * zcols, 128), zcols)]
            for d in range(1, nz):
                total += buf_c[(z + d) % nz]
            acc_c[...] = total
        elif k == 3:
            frag_b().start()
        elif k == 4:
            frag_b().wait_recv()
            rows = pl.ds(pl.multiple_of(xh * 16, 16), 16)
            mean_a[z, rows, :] = gpiece[...] - (acc_c[rows, :] + buf_b[...]) * (1.0 / reps)
        elif k == 5:
            frag_b_back().start()
        elif k == 6:
            other = mean_a.at[z, pl.ds(pl.multiple_of((1 - xh) * 16, 16), 16), :]
            rdma(other, other, fs.at[2], fr.at[2], dev_h).wait_recv()
            for d in range(1, nz):
                frag_c_back(d).start()
        elif k == 7:
            for d in range(1, nz):
                slot = mean_a.at[(z + nz - d) % nz]
                rdma(slot, slot, fds.at[d], fdr.at[d], rep_dev(xh, (z + d) % nz, core)).wait_recv()
            frag_a_back().start()
        elif k == 8:
            frag_a_back().wait_recv()

    def mean_out(zz, c):
        which, src = ((core, mean_a), (1 - core, mean_o))[c]
        return pltpu.make_async_copy(
            src.at[zz],
            mean_h.at[pl.ds(pl.multiple_of(which * 32, 32), 32), zz * zcols : (zz + 1) * zcols],
            store.at[6 + 2 * zz + c],
        )

    def gather_stage(s):
        @pl.when(s == 0)
        def _():
            frag_step(0)

        @pl.when(s == 1)
        def _():
            frag_step(1)
            units(later, relay_later)
            units(FIRST, relay_first)
            units(later, lambda i: gather(2, FIRST + i, ox, y, FIRST + i).wait_recv())

        @pl.when(s == 2)
        def _():
            frag_step(2)

        @pl.when(s == 3)
        def _():
            frag_step(3)

        @pl.when(s == 4)
        def _():
            units(later, relay_far)
            frag_step(4)
            units(FIRST, relay_other)
            frag_step(5)

            def landed(u):
                gather(0, 13 + u, cx, far, u, 0).wait_recv()
                gather(1, 13 + u, cx, far, u, 1).wait_recv()

            units(FIRST, landed)

        @pl.when(s == 5)
        def _():
            frag_step(6)
            units(later, lambda i: gather(2, 8 + i, ox, dn, FIRST + i).wait_recv())

        @pl.when(s == 6)
        def _():
            units(later, lambda i: gather(2, 11 + i, ox, up, FIRST + i).wait_recv())

        @pl.when(s == 7)
        def _():
            def landed(u):
                gather(0, 21 + u, ox, far, u, 0).wait_recv()
                gather(1, 21 + u, ox, far, u, 1).wait_recv()

            units(FIRST, landed)
            units(later, lambda i: gather(2, 14 + i, ox, far, FIRST + i).wait_recv())

        k = (s + 1) % 3
        d = 3 - 2 * k + 3 * (k * (k - 1) // 2)
        beyond = (s + 6) // 8
        row = (y + d * beyond) % 4
        other = (1 - beyond) * (s % 2) + beyond * ((s + 3) // 8)
        col = cx + other * (1 - 2 * cx)
        at = pl.ds(pl.multiple_of((col * 4 + row) * ROWS, ROWS), ROWS)
        project(at, xf[at, :], weights, table, qkv)

    units(8, gather_stage)

    attention(256, qkv, dout, table, dqkv, acc_k, acc_v)

    def scatter(way, i, src, dst):
        s, d, dev = ((rsp, rrp, dev_p), (rsm, rrm, dev_m), (rsx, rrx, dev_x))[way]
        return rdma(src, dst, s.at[i], d.at[i], dev)

    def slot(ref, i):
        return ref.at[pl.ds(pl.multiple_of(i * UNIT, UNIT), UNIT), :]

    def scatter_full(way, i, col, row, u):
        return scatter(way, i, place(part, col, row, u), slot((full_p, full_m)[way], i))

    def scatter_half(way, i, col, row, u):
        half = 1 - way
        return scatter(way, 13 + i, place(part, col, row, u, half), slot((half_p, half_m)[way], i))

    def scatter_x(i, col, row, u):
        return scatter(2, i, place(part, col, row, u), slot(from_x, i))

    def add(col, row, u, terms, half=None):
        rows = pl.ds(pl.multiple_of((col * 4 + row) * ROWS + u * UNIT, UNIT), UNIT)
        cols = slice(0, depth) if half is None else slice(half * mid, (half + 1) * mid)
        total = part[rows, cols].astype(f32)
        for ref, i in terms:
            total += ref[pl.ds(pl.multiple_of(i * UNIT, UNIT), UNIT), :].astype(f32)
        part[rows, cols] = total.astype(bf)

    def near(i, col, u):
        scatter_half(0, i, col, far, u).wait_recv()
        add(col, up, u, [(half_p, i)], 1)
        scatter_half(1, i, col, far, u).wait_recv()
        add(col, dn, u, [(half_m, i)], 0)
        scatter_full(0, i, col, up, u).start()
        scatter_full(1, i, col, dn, u).start()

    def across(i):
        scatter_full(0, i, ox, y, i).wait_recv()
        scatter_full(1, i, ox, y, i).wait_recv()
        add(ox, y, i, [(full_p, i), (full_m, i)])
        scatter_x(12 + i, ox, y, i).start()

    def far_halves(i, col, u):
        scatter_half(0, i, col, far, u).start()
        scatter_half(1, i, col, far, u).start()

    def far_later(i):
        u = FIRST + i
        scatter_x(i, cx, far, u).wait_recv()
        add(cx, far, u, [(from_x, i)])
        far_halves(5 + u, cx, u)

    def side_later(i):
        u = FIRST + i
        scatter_x(3 + i, cx, up, u).wait_recv()
        add(cx, up, u, [(from_x, 3 + i)])
        scatter_x(6 + i, cx, dn, u).wait_recv()
        add(cx, dn, u, [(from_x, 6 + i)])

    def part_stage(s):
        k = s % 4
        d = 2 - k + 3 * (k // 2) - 2 * (k // 3)
        row = (y + d) % 4
        col = ox + (s // 4) * (1 - 2 * ox)
        at = pl.ds(pl.multiple_of((col * 4 + row) * ROWS, ROWS), ROWS)
        part[at, :] = dot_t(dqkv[at, :], weights[...]).astype(bf)

        @pl.when(s < 4)
        def _():
            units(later, lambda i: scatter_x(3 * s + i, ox, row, FIRST + i).start())

        @pl.when(s == 0)
        def _():
            units(FIRST, lambda u: far_halves(u, ox, u))

        @pl.when(s == 4)
        def _():
            units(FIRST, lambda u: far_halves(5 + u, cx, u))

        @pl.when(s == 5)
        def _():
            units(FIRST, lambda u: near(u, ox, u))

        @pl.when(s == 6)
        def _():
            frag_step(7)

    units(8, part_stage)

    def weight_stage(j):
        @pl.when(j == 1)
        def _():
            units(later, far_later)

        @pl.when(j == 3)
        def _():
            units(FIRST, lambda u: near(5 + u, cx, u))

        @pl.when(j == 5)
        def _():
            units(FIRST, across)

        @pl.when(j == 7)
        def _():
            units(later, side_later)

        @pl.when(j == 8)
        def _():
            units(later, lambda i: near(5 + FIRST + i, cx, FIRST + i))

        @pl.when(j == 9)
        def _():
            frag_step(8)
            for zz in range(nz):
                for c in range(2):
                    mean_out(zz, c).start()

        block = depth // STEPS
        at = pl.ds(pl.multiple_of(j * block, block), block)
        g = t_dot(xf[:, at], dqkv[...]).astype(bf)
        gq[at, :] = g[:, :wide_q]
        gk[at, :] = g[:, wide_q : wide_q + HEAD]
        gv[at, :] = g[:, wide_q + HEAD :]

    units(STEPS, weight_stage)
    stores = [(gq, gq_h), (gk, gk_h), (gv, gv_h)]
    stores = [pltpu.make_async_copy(a, b, store.at[i]) for i, (a, b) in enumerate(stores)]
    for c in stores:
        c.start()

    gsum[...] = jnp.zeros_like(gsum)

    def finish(u):
        @pl.when(u < FIRST)
        def _():
            scatter_x(12 + u, cx, y, u).wait_recv()

        @pl.when(u >= FIRST)
        def _():
            scatter_x(9 + u - FIRST, cx, y, u).wait_recv()

        at_x = (12 + u) * (1 - u // FIRST) + (4 + u) * (u // FIRST)
        scatter_full(0, 5 + u, cx, y, u).wait_recv()
        scatter_full(1, 5 + u, cx, y, u).wait_recv()

        def term(ref, i):
            return ref[pl.ds(pl.multiple_of(i * UNIT, UNIT), UNIT), :].astype(f32)

        mine = (cx * 4 + y) * UNITS + u
        total = (term(part, mine) + term(from_x, at_x)) + (term(full_p, 5 + u) + term(full_m, 5 + u))
        rows = pl.ds(pl.multiple_of(u * UNIT, UNIT), UNIT)
        xhat, inverse = normalise(rows, tokens)
        gsum[...] += total * xhat
        scaled = total * gain[...]
        mean = jnp.mean(scaled * xhat, axis=1, keepdims=True)
        gtok[rows, :] = (inverse * (scaled - xhat * mean)).astype(bf)

    units(UNITS, finish)
    gbuf[t] = jnp.sum(gsum[...], axis=0, keepdims=True)
    out_tokens = pltpu.make_async_copy(gtok, gtok_h, store.at[3])
    out_tokens.start()

    def gain_to(d):
        return rdma(gbuf.at[t], gbuf.at[t], gs.at[d], gr.at[d], (r, (t + d) % 8))

    for d in range(1, 8):
        gain_to(d).start()
    for d in range(1, 8):
        ref = gbuf.at[(t + 8 - d) % 8]
        rdma(ref, ref, gs.at[d], gr.at[d], (r, (t + d) % 8)).wait_recv()
    total = gbuf[0]
    for d in range(1, 8):
        total += gbuf[d]
    gfin[...] = total
    out_gain = pltpu.make_async_copy(gfin, ggain_h, store.at[4])
    out_gain.start()

    units(8, lambda i: [gather(w, i, cx, y, i).wait_send() for w in range(3)] and None)
    units(FIRST, lambda i: [gather(w, 8 + i, ox, y, i).wait_send() for w in range(2)] and None)
    units(13, lambda i: [gather(w, 13 + i, cx, y, 0, w).wait_send() for w in range(2)] and None)
    units(9, lambda i: gather(2, 8 + i, cx, y, 0).wait_send())
    units(13, lambda i: [scatter_full(w, i, cx, y, 0).wait_send() for w in range(2)] and None)
    units(13, lambda i: [scatter_half(w, i, cx, y, 0).wait_send() for w in range(2)] and None)
    units(17, lambda i: scatter_x(i, cx, y, 0).wait_send())
    for d in range(1, 8):
        gain_to(d).wait_send()
    for d in range(1, nz):
        frag_c(d).wait_send()
        frag_c_back(d).wait_send()
    frag_a().wait_send()
    frag_b().wait_send()
    frag_b_back().wait_send()
    frag_a_back().wait_send()
    for c in stores + [out_tokens, out_gain]:
        c.wait()
    for zz in range(nz):
        for c in range(2):
            mean_out(zz, c).wait()


def run(reps, tokens, gain, wq, wk, wv, dout, global_fragment, local_fragment):
    depth = tokens.shape[1]
    seq = dout.shape[0]
    table = rope_constants(seq)
    f32, bf = jnp.float32, jnp.bfloat16
    cols = wq.shape[1] + wk.shape[1] + wv.shape[1]
    anywhere = pl.BlockSpec(memory_space=pl.ANY)
    nz = reps // 4
    zcols = depth // nz
    dma = pltpu.SemaphoreType.DMA
    vm = pltpu.VMEM
    scratch = [
        vm((ROWS, depth), bf), vm((1, depth), f32), vm((seq, depth), bf), vm((depth, cols), bf),
        vm((seq, cols), bf), vm((seq, cols), bf), vm(dout.shape, bf), vm(table.shape, f32),
        vm((seq, HEAD), f32), vm((seq, HEAD), f32),
        vm((seq, depth), bf),
        vm((13 * UNIT, depth), bf), vm((13 * UNIT, depth), bf),
        vm((13 * UNIT, depth // 2), bf), vm((13 * UNIT, depth // 2), bf), vm((17 * UNIT, depth), bf),
        vm(wq.shape, bf), vm(wk.shape, bf), vm(wv.shape, bf), vm((ROWS, depth), bf),
        vm((8, 1, depth), f32), vm((UNIT, depth), f32), vm((1, depth), f32),
        vm((64, depth), bf), vm((32, depth), bf), vm((32, depth), f32), vm((nz, 32, zcols), f32),
        vm((32, zcols), f32), vm((16, zcols), f32), vm((nz, 32, zcols), f32), vm((nz, 32, zcols), f32),
        vm((16, zcols), f32),
        dma((9,)), dma((6 + 2 * nz,)),
    ]
    scratch += [dma((n,)) for n in (26, 26, 17) * 4]
    scratch += [dma((n,)) for n in (8, 8, 4, 4, nz, nz, nz, nz)]
    return pl.pallas_call(
        functools.partial(step_kernel, reps),
        out_shape=(
            jax.ShapeDtypeStruct(wq.shape, bf),
            jax.ShapeDtypeStruct(wk.shape, bf),
            jax.ShapeDtypeStruct(wv.shape, bf),
            jax.ShapeDtypeStruct((1, depth), f32),
            jax.ShapeDtypeStruct((ROWS, depth), bf),
            jax.ShapeDtypeStruct((64, depth), f32),
        ),
        in_specs=[anywhere] * 9,
        out_specs=[anywhere] * 6,
        scratch_shapes=scratch,
        compiler_params=pltpu.CompilerParams(
            vmem_limit_bytes=60 * 1024 * 1024, collective_id=0, has_side_effects=True
        ),
    )(tokens, gain, wq, wk, wv, dout, table, global_fragment, local_fragment)


def body(tokens, norm_gain, w_query, key_weight, value_weight, attention_gradient, global_fragment, momentum, local_fragment):
    replicas = lax.axis_size("rep")
    gq, gk, gv, grad_gain, grad_tokens, mean = run(
        replicas, tokens[0], norm_gain, w_query[0], key_weight[0], value_weight[0],
        attention_gradient[0], global_fragment, local_fragment[0],
    )
    new_momentum = OUTER_MOMENTUM * momentum + mean
    new_global = global_fragment - OUTER_RATE * (mean + OUTER_MOMENTUM * new_momentum)
    return (gq[None], gk[None], gv[None], grad_gain, grad_tokens[None], new_global, new_momentum)


def solution(mesh):
    placed = (
        P("rep", "tp", None), P("rep", None), P("rep", None, "tp"), P("rep", None, "tp"), P("rep", None, "tp"),
        P("rep", None, "tp"), P("tp", None), P("tp", None), P("rep", "tp", None),
    )
    outs = (P("rep", None, "tp"), P("rep", None, "tp"), P("rep", None, "tp"), P("rep", None), P("rep", "tp", None), P("tp", None), P("tp", None))
    return jax.shard_map(body, mesh=mesh, in_specs=placed, out_specs=outs, check_vma=False)
```

```python
import functools

import jax
import jax.numpy as jnp
import numpy as np
from jax import lax
from jax.experimental import pallas as pl
from jax.experimental.pallas import tpu as pltpu
from jax.sharding import PartitionSpec as P

HEAD = 128
EPSILON = 1e-05
ROPE_BASE = 500000.0
OUTER_RATE = 0.7
OUTER_MOMENTUM = 0.9
NEGATIVE = -1e30


def rope_constants(seq):
    half = HEAD // 2
    freq = ROPE_BASE ** (-2.0 * np.arange(half, dtype=np.float64) / HEAD)
    angle = np.arange(seq, dtype=np.float64)[:, None] * freq[None, :]
    cos, sin = np.cos(angle), np.sin(angle)
    table = np.concatenate([cos, cos, -sin, sin], axis=1)
    return jnp.asarray(table.astype(np.float32))


def rope(v, cos, sin):
    return v * cos + pltpu.roll(v, HEAD // 2, 1) * sin


def unrope(g, cos, sin):
    return g * cos - pltpu.roll(g, HEAD // 2, 1) * sin


def project(rows, x, weights, table, qkv):
    heads = qkv.shape[1] // HEAD
    cos = table[rows, :HEAD]
    sin = table[rows, HEAD:]
    out = jnp.dot(x, weights[...], preferred_element_type=jnp.float32)
    for h in range(heads):
        part = out[:, h * HEAD : (h + 1) * HEAD]
        if h < heads - 1:
            part = rope(part, cos, sin)
        qkv[rows, h * HEAD : (h + 1) * HEAD] = part.astype(jnp.bfloat16)


def dot_t(a, b):
    return lax.dot_general(a, b, (((1,), (1,)), ((), ())), preferred_element_type=jnp.float32)


def t_dot(a, b):
    return lax.dot_general(a, b, (((0,), (0,)), ((), ())), preferred_element_type=jnp.float32)


def attention_rows(start, block, qkv, dout, table, dqkv, acc_k, acc_v, first):
    width = start + block
    scale = HEAD ** (-0.5)
    power_scale = scale * 1.4426950408889634
    heads = dout.shape[1] // HEAD
    at_k, at_v = heads * HEAD, (heads + 1) * HEAD
    keys = qkv[:width, at_k : at_k + HEAD]
    values = qkv[:width, at_v : at_v + HEAD]
    rows = slice(start, start + block)
    key = lax.broadcasted_iota(jnp.int32, (block, block), 0)
    query = lax.broadcasted_iota(jnp.int32, (block, block), 1)
    allowed = key <= query
    cos, sin = table[rows, :HEAD], table[rows, HEAD:]
    dk = dv = None
    for h in range(heads):
        q = qkv[rows, h * HEAD : (h + 1) * HEAD]
        do = dout[rows, h * HEAD : (h + 1) * HEAD]
        s = dot_t(keys, q)
        last = jnp.where(allowed, s[start:, :], NEGATIVE)
        s = last if start == 0 else jnp.concatenate([s[:start, :], last], axis=0)
        top = jnp.max(s, axis=0, keepdims=True)
        power = jnp.exp2((s - top) * power_scale)
        inverse = 1.0 / jnp.sum(power, axis=0, keepdims=True)
        p_low = (power * inverse).astype(jnp.bfloat16)
        dp = dot_t(values, do)
        drop = jnp.sum(dp * power, axis=0, keepdims=True) * inverse
        ds = (power * ((dp - drop) * (inverse * scale))).astype(jnp.bfloat16)
        dq = t_dot(keys, ds).T
        dqkv[rows, h * HEAD : (h + 1) * HEAD] = unrope(dq, cos, sin).astype(jnp.bfloat16)
        tv = jnp.dot(p_low, do, preferred_element_type=jnp.float32)
        tk = jnp.dot(ds, q, preferred_element_type=jnp.float32)
        dv = tv if dv is None else dv + tv
        dk = tk if dk is None else dk + tk
    if first:
        acc_v[:width, :] = dv
        acc_k[:width, :] = dk
    else:
        acc_v[:width, :] += dv
        acc_k[:width, :] += dk
    dqkv[rows, at_k : at_k + HEAD] = unrope(acc_k[rows, :], cos, sin).astype(jnp.bfloat16)
    dqkv[rows, at_v : at_v + HEAD] = acc_v[rows, :].astype(jnp.bfloat16)


ROWS = 128
UNIT = 16
UNITS = ROWS // UNIT
BLOCK = 256
FIRST = 5
STEPS = 12
LIMIT = 44 * 1024 * 1024


def units(count, step, start=0):
    def one(i, carry):
        step(i)
        return carry

    lax.fori_loop(start, start + count, one, 0)


def normalise(rows, tokens):
    wide = tokens[rows, :].astype(jnp.float32)
    inverse = lax.rsqrt(jnp.mean(wide * wide, axis=1, keepdims=True) + EPSILON)
    return wide * inverse, inverse


def step_kernel(
    reps,
    tokens_h, gain_h, wq_h, wk_h, wv_h, dout_h, table_h, global_h, momentum_h, local_h,
    gq, gk, gv, ggain, gtok, new_global, new_momentum,
    tokens, gain, xf, weights, qkv, dqkv, dout, table, acc_k, acc_v,
    part, full_p, full_m, half_p, half_m, from_x,
    gbuf, gsum,
    frag, buf_a, acc_a, buf_c, acc_c, buf_b, mean_a, mean_o, glob, mom,
    load,
    asp, asm, asx, arp, arm, arx,
    rsp, rsm, rsx, rrp, rrm, rrx,
    gs, gr, fs, fr, fcs, fcr, fds, fdr,
):
    f32, bf = jnp.float32, jnp.bfloat16
    depth = xf.shape[1]
    mid = depth // 2
    r, t = lax.axis_index("rep"), lax.axis_index("tp")
    nz = reps // 4
    xh, z, core = r // (2 * nz), (r // 2) % nz, r % 2
    cx, y = t // 4, t % 4
    ox = 1 - cx
    up, dn, far = (y + 1) % 4, (y + 3) % 4, (y + 2) % 4

    def tp_dev(col, row):
        return (r, col * 4 + row)

    def rep_dev(h, zz, c):
        return (h * (2 * nz) + zz * 2 + c, t)

    dev_p, dev_m, dev_x = tp_dev(cx, up), tp_dev(cx, dn), tp_dev(ox, y)
    dev_core, dev_h = rep_dev(xh, z, 1 - core), rep_dev(1 - xh, z, core)

    def rdma(src, dst, s, d, dev):
        return pltpu.make_async_remote_copy(
            src_ref=src, dst_ref=dst, send_sem=s, recv_sem=d,
            device_id=dev, device_id_type=pl.DeviceIdType.MESH,
        )

    wide_q = wq_h.shape[1]
    loads = [
        (tokens_h, tokens),
        (gain_h, gain),
        (local_h, frag),
        (wq_h, weights.at[:, :wide_q]),
        (wk_h, weights.at[:, wide_q : wide_q + HEAD]),
        (wv_h, weights.at[:, wide_q + HEAD :]),
        (table_h, table),
        (dout_h, dout),
        (global_h, glob),
        (momentum_h, mom),
    ]
    loads = [pltpu.make_async_copy(a, b, load.at[i]) for i, (a, b) in enumerate(loads)]
    for c in loads:
        c.start()

    barrier = pltpu.get_barrier_semaphore()
    peers = [(r, (t + d) % 8) for d in range(1, 8)]
    peers += [dev_core, dev_h] + [rep_dev(xh, (z + d) % nz, core) for d in range(1, nz)]
    for p in peers:
        pl.semaphore_signal(barrier, inc=1, device_id=p, device_id_type=pl.DeviceIdType.MESH)
    loads[0].wait()
    loads[1].wait()

    def norm_unit(u):
        rows = pl.ds(pl.multiple_of(u * UNIT, UNIT), UNIT)
        xhat, _ = normalise(rows, tokens)
        at = pl.ds(pl.multiple_of(t * ROWS + u * UNIT, UNIT), UNIT)
        xf[at, :] = (xhat * gain[...]).astype(bf)

    units(UNITS, norm_unit)
    loads[2].wait()
    pl.semaphore_wait(barrier, len(peers))

    def frag_a():
        other = pl.ds(pl.multiple_of((1 - core) * 32, 32), 32)
        return rdma(frag.at[other, :], buf_a, fs.at[0], fr.at[0], dev_core)

    def place(ref, col, row, u, half=None):
        rows = pl.ds(pl.multiple_of((col * 4 + row) * ROWS + u * UNIT, UNIT), UNIT)
        if half is None:
            return ref.at[rows, :]
        return ref.at[rows, half * mid : (half + 1) * mid]

    def gather(way, i, col, row, u, half=None):
        s, d, dev = ((asp, arp, dev_p), (asm, arm, dev_m), (asx, arx, dev_x))[way]
        ref = place(xf, col, row, u, half)
        return rdma(ref, ref, s.at[i], d.at[i], dev)

    def send_own(i):
        u = (i + FIRST) % UNITS
        for way in range(3):
            gather(way, u, cx, y, u).start()

    units(UNITS, send_own)
    frag_a().start()
    gsum[...] = jnp.zeros_like(gsum)
    for c in loads[3:]:
        c.wait()

    later = UNITS - FIRST

    def relay_later(i):
        u = FIRST + i
        gather(0, u, cx, dn, u).wait_recv()
        gather(0, 13 + u, cx, dn, u, 0).start()
        gather(2, 8 + i, cx, dn, u).start()
        gather(1, u, cx, up, u).wait_recv()
        gather(1, 13 + u, cx, up, u, 1).start()
        gather(2, 11 + i, cx, up, u).start()

    def relay_first(u):
        gather(0, u, cx, dn, u).wait_recv()
        gather(0, 13 + u, cx, dn, u, 0).start()
        gather(1, u, cx, up, u).wait_recv()
        gather(1, 13 + u, cx, up, u, 1).start()
        gather(2, u, ox, y, u).wait_recv()
        gather(0, 8 + u, ox, y, u).start()
        gather(1, 8 + u, ox, y, u).start()

    def relay_far(i):
        u = FIRST + i
        gather(0, 13 + u, cx, far, u, 0).wait_recv()
        gather(1, 13 + u, cx, far, u, 1).wait_recv()
        gather(2, 14 + i, cx, far, u).start()

    def relay_other(u):
        gather(0, 8 + u, ox, dn, u).wait_recv()
        gather(0, 21 + u, ox, dn, u, 0).start()
        gather(1, 8 + u, ox, up, u).wait_recv()
        gather(1, 21 + u, ox, up, u, 1).start()

    zcols = depth // nz

    def frag_c(d):
        peer = (z + d) % nz
        return rdma(
            acc_a.at[:, pl.ds(pl.multiple_of(peer * zcols, 128), zcols)], buf_c.at[z],
            fcs.at[d], fcr.at[d], rep_dev(xh, peer, core),
        )

    def frag_b():
        other = pl.ds(pl.multiple_of((1 - xh) * 16, 16), 16)
        return rdma(acc_c.at[other, :], buf_b, fs.at[1], fr.at[1], dev_h)

    def frag_b_back():
        mine = mean_a.at[z, pl.ds(pl.multiple_of(xh * 16, 16), 16), :]
        return rdma(mine, mine, fs.at[2], fr.at[2], dev_h)

    def frag_c_back(d):
        return rdma(mean_a.at[z], mean_a.at[z], fds.at[d], fdr.at[d], rep_dev(xh, (z + d) % nz, core))

    def frag_a_back():
        return rdma(mean_a, mean_o, fs.at[3], fr.at[3], dev_core)

    def frag_step(k):
        if k == 0:
            frag_a().wait_recv()
            own = frag[pl.ds(pl.multiple_of(core * 32, 32), 32), :]
            acc_a[...] = own.astype(f32) + buf_a[...].astype(f32)
        elif k == 1:
            for d in range(1, nz):
                frag_c(d).start()
        elif k == 2:
            for d in range(1, nz):
                frag_c(d).wait_recv()
            total = acc_a[:, pl.ds(pl.multiple_of(z * zcols, 128), zcols)]
            for d in range(1, nz):
                total += buf_c[(z + d) % nz]
            acc_c[...] = total
        elif k == 3:
            frag_b().start()
        elif k == 4:
            frag_b().wait_recv()
            rows = pl.ds(pl.multiple_of(xh * 16, 16), 16)
            mean_a[z, rows, :] = (
                glob[
                    pl.ds(pl.multiple_of(core * 32 + xh * 16, 16), 16),
                    pl.ds(pl.multiple_of(z * zcols, 128), zcols),
                ]
                - (acc_c[rows, :] + buf_b[...]) * (1.0 / reps)
            )
        elif k == 5:
            frag_b_back().start()
        elif k == 6:
            other = mean_a.at[z, pl.ds(pl.multiple_of((1 - xh) * 16, 16), 16), :]
            rdma(other, other, fs.at[2], fr.at[2], dev_h).wait_recv()
            for d in range(1, nz):
                frag_c_back(d).start()
        elif k == 7:
            for d in range(1, nz):
                slot = mean_a.at[(z + nz - d) % nz]
                rdma(slot, slot, fds.at[d], fdr.at[d], rep_dev(xh, (z + d) % nz, core)).wait_recv()
            frag_a_back().start()
        elif k == 8:
            frag_a_back().wait_recv()

    def outer_update(zz):
        cols = slice(zz * zcols, (zz + 1) * zcols)
        for which, src in ((core, mean_a), (1 - core, mean_o)):
            rows = pl.ds(pl.multiple_of(which * 32, 32), 32)
            mean = src[zz]
            moved = OUTER_MOMENTUM * mom[rows, cols] + mean
            new_momentum[rows, cols] = moved
            new_global[rows, cols] = glob[rows, cols] - OUTER_RATE * (mean + OUTER_MOMENTUM * moved)

    def gather_stage(s):
        @pl.when(s == 0)
        def _():
            frag_step(0)

        @pl.when(s == 1)
        def _():
            frag_step(1)
            units(later, relay_later)
            units(FIRST, relay_first)
            units(later, lambda i: gather(2, FIRST + i, ox, y, FIRST + i).wait_recv())

        @pl.when(s == 2)
        def _():
            frag_step(2)

        @pl.when(s == 3)
        def _():
            frag_step(3)

        @pl.when(s == 4)
        def _():
            units(later, relay_far)
            frag_step(4)
            units(FIRST, relay_other)
            frag_step(5)

            def landed(u):
                gather(0, 13 + u, cx, far, u, 0).wait_recv()
                gather(1, 13 + u, cx, far, u, 1).wait_recv()

            units(FIRST, landed)

        @pl.when(s == 5)
        def _():
            frag_step(6)
            units(later, lambda i: gather(2, 8 + i, ox, dn, FIRST + i).wait_recv())

        @pl.when(s == 6)
        def _():
            units(later, lambda i: gather(2, 11 + i, ox, up, FIRST + i).wait_recv())

        @pl.when(s == 7)
        def _():
            def landed(u):
                gather(0, 21 + u, ox, far, u, 0).wait_recv()
                gather(1, 21 + u, ox, far, u, 1).wait_recv()

            units(FIRST, landed)
            units(later, lambda i: gather(2, 14 + i, ox, far, FIRST + i).wait_recv())

        k = (s + 1) % 3
        d = 3 - 2 * k + 3 * (k * (k - 1) // 2)
        beyond = (s + 6) // 8
        row = (y + d * beyond) % 4
        other = (1 - beyond) * (s % 2) + beyond * ((s + 3) // 8)
        col = cx + other * (1 - 2 * cx)
        at = pl.ds(pl.multiple_of((col * 4 + row) * ROWS, ROWS), ROWS)
        project(at, xf[at, :], weights, table, qkv)

    units(8, gather_stage)

    def scatter(way, i, src, dst):
        s, d, dev = ((rsp, rrp, dev_p), (rsm, rrm, dev_m), (rsx, rrx, dev_x))[way]
        return rdma(src, dst, s.at[i], d.at[i], dev)

    def slot(ref, i):
        return ref.at[pl.ds(pl.multiple_of(i * UNIT, UNIT), UNIT), :]

    def scatter_full(way, i, col, row, u):
        return scatter(way, i, place(part, col, row, u), slot((full_p, full_m)[way], i))

    def scatter_half(way, i, col, row, u):
        half = 1 - way
        return scatter(way, 13 + i, place(part, col, row, u, half), slot((half_p, half_m)[way], i))

    def scatter_x(i, col, row, u):
        return scatter(2, i, place(part, col, row, u), slot(from_x, i))

    def add(col, row, u, terms, half=None):
        rows = pl.ds(pl.multiple_of((col * 4 + row) * ROWS + u * UNIT, UNIT), UNIT)
        cols = slice(0, depth) if half is None else slice(half * mid, (half + 1) * mid)
        total = part[rows, cols].astype(f32)
        for ref, i in terms:
            total += ref[pl.ds(pl.multiple_of(i * UNIT, UNIT), UNIT), :].astype(f32)
        part[rows, cols] = total.astype(bf)

    def near(i, col, u):
        scatter_half(0, i, col, far, u).wait_recv()
        add(col, up, u, [(half_p, i)], 1)
        scatter_half(1, i, col, far, u).wait_recv()
        add(col, dn, u, [(half_m, i)], 0)
        scatter_full(0, i, col, up, u).start()
        scatter_full(1, i, col, dn, u).start()

    def across(i):
        scatter_full(0, i, ox, y, i).wait_recv()
        scatter_full(1, i, ox, y, i).wait_recv()
        add(ox, y, i, [(full_p, i), (full_m, i)])
        scatter_x(12 + i, ox, y, i).start()

    def far_halves(i, col, u):
        scatter_half(0, i, col, far, u).start()
        scatter_half(1, i, col, far, u).start()

    def far_later(i):
        u = FIRST + i
        scatter_x(3 + i, cx, far, u).wait_recv()
        add(cx, far, u, [(from_x, 3 + i)])
        far_halves(5 + u, cx, u)

    def side_later(i):
        u = FIRST + i
        scatter_x(i, cx, up, u).wait_recv()
        add(cx, up, u, [(from_x, i)])
        scatter_x(6 + i, cx, dn, u).wait_recv()
        add(cx, dn, u, [(from_x, 6 + i)])

    def terms(chunk):
        col, row = chunk // 4, chunk % 4
        away = (row + 4 - y) % 4
        other = (col + cx) % 2
        at = pl.ds(pl.multiple_of(chunk * ROWS, ROWS), ROWS)
        width = min(512, depth)
        for j in range(0, depth, width):
            cols = slice(j, j + width)
            low = dot_t(dqkv[at, :], weights[cols, :]).astype(bf)
            part[at, cols] = low
            moved = low.astype(f32) * xf[at, cols].astype(f32)
            gsum[:, cols] += jnp.sum(moved.reshape(ROWS // 8, 8, width), axis=0)

        @pl.when(other == 1)
        def _():
            role = (away + 3) % 4
            units(later, lambda i: scatter_x(3 * role + i, ox, row, FIRST + i).start())

        @pl.when(away == 2)
        def _():
            units(FIRST, lambda u: far_halves(5 * (1 - other) + u, col, u))

    seq = qkv.shape[0]
    for start in reversed(range(0, seq, BLOCK)):
        attention_rows(start, BLOCK, qkv, dout, table, dqkv, acc_k, acc_v, start + BLOCK == seq)
        count = BLOCK // ROWS
        units(count, lambda i: terms(start // ROWS + count - 1 - i))

    gbuf[t] = jnp.sum(gsum[...], axis=0, keepdims=True)
    units(FIRST, lambda u: near(u, ox, u))

    def gain_to(d):
        return rdma(gbuf.at[t], gbuf.at[t], gs.at[d], gr.at[d], (r, (t + d) % 8))

    for d in range(1, 8):
        gain_to(d).start()
    frag_step(7)

    def weight_stage(j):
        @pl.when(j == 1)
        def _():
            units(later, far_later)

        @pl.when(j == 3)
        def _():
            units(FIRST, lambda u: near(5 + u, cx, u))

        @pl.when(j == 5)
        def _():
            units(FIRST, across)

        @pl.when(j == 7)
        def _():
            units(later, side_later)

        @pl.when(j == 8)
        def _():
            units(later, lambda i: near(5 + FIRST + i, cx, FIRST + i))

        @pl.when(j == 9)
        def _():
            frag_step(8)
            for zz in range(nz):
                outer_update(zz)

        @pl.when(j == 10)
        def _():
            for d in range(1, 8):
                ref = gbuf.at[(t + 8 - d) % 8]
                rdma(ref, ref, gs.at[d], gr.at[d], (r, (t + d) % 8)).wait_recv()
            total = gbuf[0]
            for d in range(1, 8):
                total += gbuf[d]
            ggain[...] = total / gain[...]

        block = depth // STEPS
        at = pl.ds(pl.multiple_of(j * block, block), block)
        g = t_dot(xf[:, at], dqkv[...]).astype(bf)
        gq[at, :] = g[:, :wide_q]
        gk[at, :] = g[:, wide_q : wide_q + HEAD]
        gv[at, :] = g[:, wide_q + HEAD :]

    units(STEPS, weight_stage)

    def finish(u):
        @pl.when(u < FIRST)
        def _():
            scatter_x(12 + u, cx, y, u).wait_recv()

        @pl.when(u >= FIRST)
        def _():
            scatter_x(9 + u - FIRST, cx, y, u).wait_recv()

        at_x = (12 + u) * (1 - u // FIRST) + (4 + u) * (u // FIRST)
        scatter_full(0, 5 + u, cx, y, u).wait_recv()
        scatter_full(1, 5 + u, cx, y, u).wait_recv()

        def term(ref, i):
            return ref[pl.ds(pl.multiple_of(i * UNIT, UNIT), UNIT), :].astype(f32)

        mine = (cx * 4 + y) * UNITS + u
        total = (term(part, mine) + term(from_x, at_x)) + (term(full_p, 5 + u) + term(full_m, 5 + u))
        rows = pl.ds(pl.multiple_of(u * UNIT, UNIT), UNIT)
        xhat, inverse = normalise(rows, tokens)
        scaled = total * gain[...]
        mean = jnp.mean(scaled * xhat, axis=1, keepdims=True)
        gtok[rows, :] = (inverse * (scaled - xhat * mean)).astype(bf)

    units(UNITS, finish)

    units(8, lambda i: [gather(w, i, cx, y, i).wait_send() for w in range(3)] and None)
    units(FIRST, lambda i: [gather(w, 8 + i, ox, y, i).wait_send() for w in range(2)] and None)
    units(13, lambda i: [gather(w, 13 + i, cx, y, 0, w).wait_send() for w in range(2)] and None)
    units(9, lambda i: gather(2, 8 + i, cx, y, 0).wait_send())
    units(13, lambda i: [scatter_full(w, i, cx, y, 0).wait_send() for w in range(2)] and None)
    units(13, lambda i: [scatter_half(w, i, cx, y, 0).wait_send() for w in range(2)] and None)
    units(17, lambda i: scatter_x(i, cx, y, 0).wait_send())
    for d in range(1, 8):
        gain_to(d).wait_send()
    for d in range(1, nz):
        frag_c(d).wait_send()
        frag_c_back(d).wait_send()
    frag_a().wait_send()
    frag_b().wait_send()
    frag_b_back().wait_send()
    frag_a_back().wait_send()


def run(reps, tokens, gain, wq, wk, wv, dout, global_fragment, momentum, local_fragment):
    depth = tokens.shape[1]
    seq = dout.shape[0]
    table = rope_constants(seq)
    f32, bf = jnp.float32, jnp.bfloat16
    cols = wq.shape[1] + wk.shape[1] + wv.shape[1]
    anywhere = pl.BlockSpec(memory_space=pltpu.HBM)
    nz = reps // 4
    zcols = depth // nz
    dma = pltpu.SemaphoreType.DMA
    vm = pltpu.VMEM
    scratch = [
        vm((ROWS, depth), bf), vm((1, depth), f32), vm((seq, depth), bf), vm((depth, cols), bf),
        vm((seq, cols), bf), vm((seq, cols), bf), vm(dout.shape, bf), vm(table.shape, f32),
        vm((seq, HEAD), f32), vm((seq, HEAD), f32),
        vm((seq, depth), bf),
        vm((13 * UNIT, depth), bf), vm((13 * UNIT, depth), bf),
        vm((13 * UNIT, depth // 2), bf), vm((13 * UNIT, depth // 2), bf), vm((17 * UNIT, depth), bf),
        vm((8, 1, depth), f32), vm((8, depth), f32),
        vm((64, depth), bf), vm((32, depth), bf), vm((32, depth), f32), vm((nz, 32, zcols), f32),
        vm((32, zcols), f32), vm((16, zcols), f32), vm((nz, 32, zcols), f32), vm((nz, 32, zcols), f32),
        vm((64, depth), f32), vm((64, depth), f32),
        dma((10,)),
    ]
    scratch += [dma((n,)) for n in (26, 26, 17) * 4]
    scratch += [dma((n,)) for n in (8, 8, 4, 4, nz, nz, nz, nz)]
    operands = (tokens, gain, wq, wk, wv, dout, table, global_fragment, momentum, local_fragment)
    return pl.pallas_call(
        functools.partial(step_kernel, reps),
        out_shape=(
            jax.ShapeDtypeStruct(wq.shape, bf),
            jax.ShapeDtypeStruct(wk.shape, bf),
            jax.ShapeDtypeStruct(wv.shape, bf),
            jax.ShapeDtypeStruct((1, depth), f32),
            jax.ShapeDtypeStruct((ROWS, depth), bf),
            jax.ShapeDtypeStruct((64, depth), f32),
            jax.ShapeDtypeStruct((64, depth), f32),
        ),
        in_specs=[anywhere] * 10,
        out_specs=[pl.BlockSpec(memory_space=pltpu.VMEM)] * 7,
        scratch_shapes=scratch,
        compiler_params=pltpu.CompilerParams(
            vmem_limit_bytes=LIMIT, collective_id=0, has_side_effects=True
        ),
    )(*(pltpu.with_memory_space_constraint(a, pltpu.HBM) for a in operands))


def body(tokens, norm_gain, w_query, key_weight, value_weight, attention_gradient, global_fragment, momentum, local_fragment):
    replicas = lax.axis_size("rep")
    gq, gk, gv, grad_gain, grad_tokens, new_global, new_momentum = run(
        replicas, tokens[0], norm_gain, w_query[0], key_weight[0], value_weight[0],
        attention_gradient[0], global_fragment, momentum, local_fragment[0],
    )
    return (gq[None], gk[None], gv[None], grad_gain, grad_tokens[None], new_global, new_momentum)


def solution(mesh):
    placed = (
        P("rep", "tp", None), P("rep", None), P("rep", None, "tp"), P("rep", None, "tp"), P("rep", None, "tp"),
        P("rep", None, "tp"), P("tp", None), P("tp", None), P("rep", "tp", None),
    )
    outs = (P("rep", None, "tp"), P("rep", None, "tp"), P("rep", None, "tp"), P("rep", None), P("rep", "tp", None), P("tp", None), P("tp", None))
    return jax.shard_map(body, mesh=mesh, in_specs=placed, out_specs=outs, check_vma=False)
```

```python
import functools

import jax
import jax.numpy as jnp
import numpy as np
from jax import lax
from jax.experimental import pallas as pl
from jax.experimental.pallas import tpu as pltpu
from jax.sharding import PartitionSpec as P

HEAD = 128
EPSILON = 1e-05
ROPE_BASE = 500000.0
OUTER_RATE = 0.7
OUTER_MOMENTUM = 0.9
NEGATIVE = -1e30


def rope_constants(seq):
    half = HEAD // 2
    freq = ROPE_BASE ** (-2.0 * np.arange(half, dtype=np.float64) / HEAD)
    angle = np.arange(seq, dtype=np.float64)[:, None] * freq[None, :]
    cos, sin = np.cos(angle), np.sin(angle)
    table = np.concatenate([cos, cos, -sin, sin], axis=1)
    return jnp.asarray(table.astype(np.float32))


def rope(v, cos, sin):
    return v * cos + pltpu.roll(v, HEAD // 2, 1) * sin


def unrope(g, cos, sin):
    return g * cos - pltpu.roll(g, HEAD // 2, 1) * sin


def project(rows, x, weights, table, qkv):
    heads = qkv.shape[1] // HEAD
    cos = table[rows, :HEAD]
    sin = table[rows, HEAD:]
    out = jnp.dot(x, weights[...], preferred_element_type=jnp.float32)
    for h in range(heads):
        part = out[:, h * HEAD : (h + 1) * HEAD]
        if h < heads - 1:
            part = rope(part, cos, sin)
        qkv[rows, h * HEAD : (h + 1) * HEAD] = part.astype(jnp.bfloat16)


def dot_t(a, b):
    return lax.dot_general(a, b, (((1,), (1,)), ((), ())), preferred_element_type=jnp.float32)


def t_dot(a, b):
    return lax.dot_general(a, b, (((0,), (0,)), ((), ())), preferred_element_type=jnp.float32)


def attention_rows(start, block, qkv, dout, table, dqkv, acc_k, acc_v, first):
    width = start + block
    scale = HEAD ** (-0.5)
    power_scale = scale * 1.4426950408889634
    heads = dout.shape[1] // HEAD
    at_k, at_v = heads * HEAD, (heads + 1) * HEAD
    keys = qkv[:width, at_k : at_k + HEAD]
    values = qkv[:width, at_v : at_v + HEAD]
    rows = slice(start, start + block)
    key = lax.broadcasted_iota(jnp.int32, (block, block), 0)
    query = lax.broadcasted_iota(jnp.int32, (block, block), 1)
    allowed = key <= query
    cos, sin = table[rows, :HEAD], table[rows, HEAD:]
    dk = dv = None
    for h in range(heads):
        q = qkv[rows, h * HEAD : (h + 1) * HEAD]
        do = dout[rows, h * HEAD : (h + 1) * HEAD]
        s = dot_t(keys, q)
        last = jnp.where(allowed, s[start:, :], NEGATIVE)
        s = last if start == 0 else jnp.concatenate([s[:start, :], last], axis=0)
        top = jnp.max(s, axis=0, keepdims=True)
        power = jnp.exp2((s - top) * power_scale)
        inverse = 1.0 / jnp.sum(power, axis=0, keepdims=True)
        p_low = (power * inverse).astype(jnp.bfloat16)
        dp = dot_t(values, do)
        drop = jnp.sum(dp * power, axis=0, keepdims=True) * inverse
        ds = (power * ((dp - drop) * (inverse * scale))).astype(jnp.bfloat16)
        dq = t_dot(keys, ds).T
        dqkv[rows, h * HEAD : (h + 1) * HEAD] = unrope(dq, cos, sin).astype(jnp.bfloat16)
        tv = jnp.dot(p_low, do, preferred_element_type=jnp.float32)
        tk = jnp.dot(ds, q, preferred_element_type=jnp.float32)
        dv = tv if dv is None else dv + tv
        dk = tk if dk is None else dk + tk
    if first:
        acc_v[:width, :] = dv
        acc_k[:width, :] = dk
    else:
        acc_v[:width, :] += dv
        acc_k[:width, :] += dk
    dqkv[rows, at_k : at_k + HEAD] = unrope(acc_k[rows, :], cos, sin).astype(jnp.bfloat16)
    dqkv[rows, at_v : at_v + HEAD] = acc_v[rows, :].astype(jnp.bfloat16)


ROWS = 128
UNIT = 16
UNITS = ROWS // UNIT
BLOCK = 256
FIRST = 5
STEPS = 12
LIMIT = 44 * 1024 * 1024


def units(count, step, start=0):
    def one(i, carry):
        step(i)
        return carry

    lax.fori_loop(start, start + count, one, 0)


def normalise(rows, tokens):
    wide = tokens[rows, :].astype(jnp.float32)
    inverse = lax.rsqrt(jnp.mean(wide * wide, axis=1, keepdims=True) + EPSILON)
    return wide * inverse, inverse


def step_kernel(
    reps,
    tokens_h, gain_h, wq_h, wk_h, wv_h, dout_h, table_h, global_h, momentum_h, local_h,
    gq, gk, gv, ggain, gtok, new_global, new_momentum,
    tokens, gain, xf, weights, qkv, dqkv, dout, table, acc_k, acc_v,
    part, full_p, full_m, half_p, half_m, from_x,
    gbuf, gsum,
    frag, buf_a, acc_a, buf_c, acc_c, buf_b, mean_a, mean_o, glob, mom,
    load,
    asp, asm, asx, arp, arm, arx,
    rsp, rsm, rsx, rrp, rrm, rrx,
    gs, gr, fs, fr, fcs, fcr, fds, fdr,
):
    f32, bf = jnp.float32, jnp.bfloat16
    depth = xf.shape[1]
    mid = depth // 2
    r, t = lax.axis_index("rep"), lax.axis_index("tp")
    nz = reps // 4
    xh, z, core = r // (2 * nz), (r // 2) % nz, r % 2
    cx, y = t // 4, t % 4
    ox = 1 - cx
    up, dn, far = (y + 1) % 4, (y + 3) % 4, (y + 2) % 4

    def tp_dev(col, row):
        return (r, col * 4 + row)

    def rep_dev(h, zz, c):
        return (h * (2 * nz) + zz * 2 + c, t)

    dev_p, dev_m, dev_x = tp_dev(cx, up), tp_dev(cx, dn), tp_dev(ox, y)
    dev_core, dev_h = rep_dev(xh, z, 1 - core), rep_dev(1 - xh, z, core)

    def rdma(src, dst, s, d, dev):
        return pltpu.make_async_remote_copy(
            src_ref=src, dst_ref=dst, send_sem=s, recv_sem=d,
            device_id=dev, device_id_type=pl.DeviceIdType.MESH,
        )

    wide_q = wq_h.shape[1]
    loads = [
        (tokens_h, tokens),
        (gain_h, gain),
        (local_h, frag),
        (wq_h, weights.at[:, :wide_q]),
        (wk_h, weights.at[:, wide_q : wide_q + HEAD]),
        (wv_h, weights.at[:, wide_q + HEAD :]),
        (table_h, table),
        (dout_h, dout),
        (global_h, glob),
        (momentum_h, mom),
    ]
    loads = [pltpu.make_async_copy(a, b, load.at[i]) for i, (a, b) in enumerate(loads)]
    for c in loads:
        c.start()

    barrier = pltpu.get_barrier_semaphore()
    peers = [(r, (t + d) % 8) for d in range(1, 8)]
    peers += [dev_core, dev_h] + [rep_dev(xh, (z + d) % nz, core) for d in range(1, nz)]
    for p in peers:
        pl.semaphore_signal(barrier, inc=1, device_id=p, device_id_type=pl.DeviceIdType.MESH)
    loads[0].wait()
    loads[1].wait()

    def norm_unit(u):
        rows = pl.ds(pl.multiple_of(u * UNIT, UNIT), UNIT)
        xhat, _ = normalise(rows, tokens)
        at = pl.ds(pl.multiple_of(t * ROWS + u * UNIT, UNIT), UNIT)
        xf[at, :] = (xhat * gain[...]).astype(bf)

    units(UNITS, norm_unit)
    loads[2].wait()
    pl.semaphore_wait(barrier, len(peers))

    def frag_a():
        other = pl.ds(pl.multiple_of((1 - core) * 32, 32), 32)
        return rdma(frag.at[other, :], buf_a, fs.at[0], fr.at[0], dev_core)

    def place(ref, col, row, u, half=None):
        rows = pl.ds(pl.multiple_of((col * 4 + row) * ROWS + u * UNIT, UNIT), UNIT)
        if half is None:
            return ref.at[rows, :]
        return ref.at[rows, half * mid : (half + 1) * mid]

    def gather(way, i, col, row, u, half=None):
        s, d, dev = ((asp, arp, dev_p), (asm, arm, dev_m), (asx, arx, dev_x))[way]
        ref = place(xf, col, row, u, half)
        return rdma(ref, ref, s.at[i], d.at[i], dev)

    def send_own(i):
        u = (i + FIRST) % UNITS
        for way in range(3):
            gather(way, u, cx, y, u).start()

    units(UNITS, send_own)
    frag_a().start()
    gsum[...] = jnp.zeros_like(gsum)
    for c in loads[3:]:
        c.wait()

    later = UNITS - FIRST

    def relay_later(i):
        u = FIRST + i
        gather(0, u, cx, dn, u).wait_recv()
        gather(0, 13 + u, cx, dn, u, 0).start()
        gather(2, 8 + i, cx, dn, u).start()
        gather(1, u, cx, up, u).wait_recv()
        gather(1, 13 + u, cx, up, u, 1).start()
        gather(2, 11 + i, cx, up, u).start()

    def relay_first(u):
        gather(0, u, cx, dn, u).wait_recv()
        gather(0, 13 + u, cx, dn, u, 0).start()
        gather(1, u, cx, up, u).wait_recv()
        gather(1, 13 + u, cx, up, u, 1).start()
        gather(2, u, ox, y, u).wait_recv()
        gather(0, 8 + u, ox, y, u).start()
        gather(1, 8 + u, ox, y, u).start()

    def relay_far(i):
        u = FIRST + i
        gather(0, 13 + u, cx, far, u, 0).wait_recv()
        gather(1, 13 + u, cx, far, u, 1).wait_recv()
        gather(2, 14 + i, cx, far, u).start()

    def relay_other(u):
        gather(0, 8 + u, ox, dn, u).wait_recv()
        gather(0, 21 + u, ox, dn, u, 0).start()
        gather(1, 8 + u, ox, up, u).wait_recv()
        gather(1, 21 + u, ox, up, u, 1).start()

    zcols = depth // nz

    def frag_c(d):
        peer = (z + d) % nz
        return rdma(
            acc_a.at[:, pl.ds(pl.multiple_of(peer * zcols, 128), zcols)], buf_c.at[z],
            fcs.at[d], fcr.at[d], rep_dev(xh, peer, core),
        )

    def frag_b():
        other = pl.ds(pl.multiple_of((1 - xh) * 16, 16), 16)
        return rdma(acc_c.at[other, :], buf_b, fs.at[1], fr.at[1], dev_h)

    def frag_b_back():
        mine = mean_a.at[z, pl.ds(pl.multiple_of(xh * 16, 16), 16), :]
        return rdma(mine, mine, fs.at[2], fr.at[2], dev_h)

    def frag_c_back(d):
        return rdma(mean_a.at[z], mean_a.at[z], fds.at[d], fdr.at[d], rep_dev(xh, (z + d) % nz, core))

    def frag_a_back():
        return rdma(mean_a, mean_o, fs.at[3], fr.at[3], dev_core)

    def frag_step(k):
        if k == 0:
            frag_a().wait_recv()
            own = frag[pl.ds(pl.multiple_of(core * 32, 32), 32), :]
            acc_a[...] = own.astype(f32) + buf_a[...].astype(f32)
        elif k == 1:
            for d in range(1, nz):
                frag_c(d).start()
        elif k == 2:
            for d in range(1, nz):
                frag_c(d).wait_recv()
            total = acc_a[:, pl.ds(pl.multiple_of(z * zcols, 128), zcols)]
            for d in range(1, nz):
                total += buf_c[(z + d) % nz]
            acc_c[...] = total
        elif k == 3:
            frag_b().start()
        elif k == 4:
            frag_b().wait_recv()
            rows = pl.ds(pl.multiple_of(xh * 16, 16), 16)
            mean_a[z, rows, :] = (
                glob[
                    pl.ds(pl.multiple_of(core * 32 + xh * 16, 16), 16),
                    pl.ds(pl.multiple_of(z * zcols, 128), zcols),
                ]
                - (acc_c[rows, :] + buf_b[...]) * (1.0 / reps)
            )
        elif k == 5:
            frag_b_back().start()
        elif k == 6:
            other = mean_a.at[z, pl.ds(pl.multiple_of((1 - xh) * 16, 16), 16), :]
            rdma(other, other, fs.at[2], fr.at[2], dev_h).wait_recv()
            for d in range(1, nz):
                frag_c_back(d).start()
        elif k == 7:
            for d in range(1, nz):
                slot = mean_a.at[(z + nz - d) % nz]
                rdma(slot, slot, fds.at[d], fdr.at[d], rep_dev(xh, (z + d) % nz, core)).wait_recv()
            frag_a_back().start()
        elif k == 8:
            frag_a_back().wait_recv()

    def outer_update(zz):
        cols = slice(zz * zcols, (zz + 1) * zcols)
        for which, src in ((core, mean_a), (1 - core, mean_o)):
            rows = pl.ds(pl.multiple_of(which * 32, 32), 32)
            mean = src[zz]
            moved = OUTER_MOMENTUM * mom[rows, cols] + mean
            new_momentum[rows, cols] = moved
            new_global[rows, cols] = glob[rows, cols] - OUTER_RATE * (mean + OUTER_MOMENTUM * moved)

    def gather_stage(s):
        @pl.when(s == 0)
        def _():
            frag_step(0)

        @pl.when(s == 1)
        def _():
            frag_step(1)
            units(later, relay_later)
            units(FIRST, relay_first)
            units(later, lambda i: gather(2, FIRST + i, ox, y, FIRST + i).wait_recv())

        @pl.when(s == 2)
        def _():
            frag_step(2)

        @pl.when(s == 3)
        def _():
            frag_step(3)

        @pl.when(s == 4)
        def _():
            units(later, relay_far)
            frag_step(4)
            units(FIRST, relay_other)
            frag_step(5)

            def landed(u):
                gather(0, 13 + u, cx, far, u, 0).wait_recv()
                gather(1, 13 + u, cx, far, u, 1).wait_recv()

            units(FIRST, landed)

        @pl.when(s == 5)
        def _():
            frag_step(6)
            units(later, lambda i: gather(2, 8 + i, ox, dn, FIRST + i).wait_recv())

        @pl.when(s == 6)
        def _():
            units(later, lambda i: gather(2, 11 + i, ox, up, FIRST + i).wait_recv())

        @pl.when(s == 7)
        def _():
            def landed(u):
                gather(0, 21 + u, ox, far, u, 0).wait_recv()
                gather(1, 21 + u, ox, far, u, 1).wait_recv()

            units(FIRST, landed)
            units(later, lambda i: gather(2, 14 + i, ox, far, FIRST + i).wait_recv())

        k = (s + 1) % 3
        d = 3 - 2 * k + 3 * (k * (k - 1) // 2)
        beyond = (s + 6) // 8
        row = (y + d * beyond) % 4
        other = (1 - beyond) * (s % 2) + beyond * ((s + 3) // 8)
        col = cx + other * (1 - 2 * cx)
        at = pl.ds(pl.multiple_of((col * 4 + row) * ROWS, ROWS), ROWS)
        project(at, xf[at, :], weights, table, qkv)

    units(8, gather_stage)

    def scatter(way, i, src, dst):
        s, d, dev = ((rsp, rrp, dev_p), (rsm, rrm, dev_m), (rsx, rrx, dev_x))[way]
        return rdma(src, dst, s.at[i], d.at[i], dev)

    def slot(ref, i):
        return ref.at[pl.ds(pl.multiple_of(i * UNIT, UNIT), UNIT), :]

    def scatter_full(way, i, col, row, u):
        return scatter(way, i, place(part, col, row, u), slot((full_p, full_m)[way], i))

    def scatter_half(way, i, col, row, u):
        half = 1 - way
        return scatter(way, 13 + i, place(part, col, row, u, half), slot((half_p, half_m)[way], i))

    def scatter_x(i, col, row, u):
        return scatter(2, i, place(part, col, row, u), slot(from_x, i))

    def add(col, row, u, terms, half=None):
        rows = pl.ds(pl.multiple_of((col * 4 + row) * ROWS + u * UNIT, UNIT), UNIT)
        cols = slice(0, depth) if half is None else slice(half * mid, (half + 1) * mid)
        total = part[rows, cols].astype(f32)
        for ref, i in terms:
            total += ref[pl.ds(pl.multiple_of(i * UNIT, UNIT), UNIT), :].astype(f32)
        part[rows, cols] = total.astype(bf)

    def near(i, col, u):
        scatter_half(0, i, col, far, u).wait_recv()
        add(col, up, u, [(half_p, i)], 1)
        scatter_half(1, i, col, far, u).wait_recv()
        add(col, dn, u, [(half_m, i)], 0)
        scatter_full(0, i, col, up, u).start()
        scatter_full(1, i, col, dn, u).start()

    def across(i):
        scatter_full(0, i, ox, y, i).wait_recv()
        scatter_full(1, i, ox, y, i).wait_recv()
        add(ox, y, i, [(full_p, i), (full_m, i)])
        scatter_x(12 + i, ox, y, i).start()

    def far_halves(i, col, u):
        scatter_half(0, i, col, far, u).start()
        scatter_half(1, i, col, far, u).start()

    def far_later(i):
        u = FIRST + i
        scatter_x(3 + i, cx, far, u).wait_recv()
        add(cx, far, u, [(from_x, 3 + i)])
        far_halves(5 + u, cx, u)

    def side_later(i):
        u = FIRST + i
        scatter_x(i, cx, up, u).wait_recv()
        add(cx, up, u, [(from_x, i)])
        scatter_x(6 + i, cx, dn, u).wait_recv()
        add(cx, dn, u, [(from_x, 6 + i)])

    def terms(chunk):
        col, row = chunk // 4, chunk % 4
        away = (row + 4 - y) % 4
        other = (col + cx) % 2
        at = pl.ds(pl.multiple_of(chunk * ROWS, ROWS), ROWS)
        width = min(512, depth)
        for j in range(0, depth, width):
            cols = slice(j, j + width)
            low = dot_t(dqkv[at, :], weights[cols, :]).astype(bf)
            part[at, cols] = low
            moved = low.astype(f32) * xf[at, cols].astype(f32)
            gsum[:, cols] += jnp.sum(moved.reshape(ROWS // 8, 8, width), axis=0)

        @pl.when(other == 1)
        def _():
            role = (away + 3) % 4
            units(later, lambda i: scatter_x(3 * role + i, ox, row, FIRST + i).start())

        @pl.when(away == 2)
        def _():
            units(FIRST, lambda u: far_halves(5 * (1 - other) + u, col, u))

    def after_3(i):
        terms(6 + (far + i) % 2)

    def after_2(i):
        terms((1 - cx) * (4 + (far + i) % 2) + cx * (4 + far))

    def after_1(i):
        terms(2 + (far + i) % 2)

    def after_0(i):
        own = 1 - cx * (1 - (i + 2) // 4)
        k = (i - cx) * own
        d = 2 - k + 3 * (k // 2) - 2 * (k // 3)
        terms(own * (cx * 4 + (y + d) % 4) + (1 - own) * ((far + i) % 2))

        @pl.when(i == 1 + 3 * cx)
        def _():
            units(FIRST, lambda u: near(u, ox, u))

    seq = qkv.shape[0]
    after = ((after_0, 4 + cx), (after_1, 2 * cx), (after_2, 2 - cx), (after_3, 2 * (1 - cx)))
    for b in reversed(range(4)):
        start = b * BLOCK
        attention_rows(start, BLOCK, qkv, dout, table, dqkv, acc_k, acc_v, start + BLOCK == seq)
        units(after[b][1], after[b][0])

    gbuf[t] = jnp.sum(gsum[...], axis=0, keepdims=True)
    def gain_to(d):
        return rdma(gbuf.at[t], gbuf.at[t], gs.at[d], gr.at[d], (r, (t + d) % 8))

    for d in range(1, 8):
        gain_to(d).start()
    frag_step(7)

    def weight_stage(j):
        @pl.when(j == 0)
        def _():
            units(3, lambda u: near(5 + u, cx, u))

        @pl.when(j == 3)
        def _():
            units(FIRST, across)

        @pl.when(j == 5)
        def _():
            units(later, far_later)
            units(FIRST - 3, lambda u: near(5 + u, cx, u), 3)

        @pl.when(j == 7)
        def _():
            units(later, side_later)

        @pl.when(j == 8)
        def _():
            units(later, lambda i: near(5 + FIRST + i, cx, FIRST + i))

        @pl.when(j == 9)
        def _():
            frag_step(8)
            for zz in range(nz):
                outer_update(zz)

        @pl.when(j == 10)
        def _():
            for d in range(1, 8):
                ref = gbuf.at[(t + 8 - d) % 8]
                rdma(ref, ref, gs.at[d], gr.at[d], (r, (t + d) % 8)).wait_recv()
            total = gbuf[0]
            for d in range(1, 8):
                total += gbuf[d]
            ggain[...] = total / gain[...]

        block = depth // STEPS
        at = pl.ds(pl.multiple_of(j * block, block), block)
        g = t_dot(xf[:, at], dqkv[...]).astype(bf)
        gq[at, :] = g[:, :wide_q]
        gk[at, :] = g[:, wide_q : wide_q + HEAD]
        gv[at, :] = g[:, wide_q + HEAD :]

    units(STEPS, weight_stage)

    def finish(u):
        @pl.when(u < FIRST)
        def _():
            scatter_x(12 + u, cx, y, u).wait_recv()

        @pl.when(u >= FIRST)
        def _():
            scatter_x(9 + u - FIRST, cx, y, u).wait_recv()

        at_x = (12 + u) * (1 - u // FIRST) + (4 + u) * (u // FIRST)
        scatter_full(0, 5 + u, cx, y, u).wait_recv()
        scatter_full(1, 5 + u, cx, y, u).wait_recv()

        def term(ref, i):
            return ref[pl.ds(pl.multiple_of(i * UNIT, UNIT), UNIT), :].astype(f32)

        mine = (cx * 4 + y) * UNITS + u
        total = (term(part, mine) + term(from_x, at_x)) + (term(full_p, 5 + u) + term(full_m, 5 + u))
        rows = pl.ds(pl.multiple_of(u * UNIT, UNIT), UNIT)
        xhat, inverse = normalise(rows, tokens)
        scaled = total * gain[...]
        mean = jnp.mean(scaled * xhat, axis=1, keepdims=True)
        gtok[rows, :] = (inverse * (scaled - xhat * mean)).astype(bf)

    units(UNITS, finish)

    units(8, lambda i: [gather(w, i, cx, y, i).wait_send() for w in range(3)] and None)
    units(FIRST, lambda i: [gather(w, 8 + i, ox, y, i).wait_send() for w in range(2)] and None)
    units(13, lambda i: [gather(w, 13 + i, cx, y, 0, w).wait_send() for w in range(2)] and None)
    units(9, lambda i: gather(2, 8 + i, cx, y, 0).wait_send())
    units(13, lambda i: [scatter_full(w, i, cx, y, 0).wait_send() for w in range(2)] and None)
    units(13, lambda i: [scatter_half(w, i, cx, y, 0).wait_send() for w in range(2)] and None)
    units(17, lambda i: scatter_x(i, cx, y, 0).wait_send())
    for d in range(1, 8):
        gain_to(d).wait_send()
    for d in range(1, nz):
        frag_c(d).wait_send()
        frag_c_back(d).wait_send()
    frag_a().wait_send()
    frag_b().wait_send()
    frag_b_back().wait_send()
    frag_a_back().wait_send()


def run(reps, tokens, gain, wq, wk, wv, dout, global_fragment, momentum, local_fragment):
    depth = tokens.shape[1]
    seq = dout.shape[0]
    table = rope_constants(seq)
    f32, bf = jnp.float32, jnp.bfloat16
    cols = wq.shape[1] + wk.shape[1] + wv.shape[1]
    anywhere = pl.BlockSpec(memory_space=pltpu.HBM)
    nz = reps // 4
    zcols = depth // nz
    dma = pltpu.SemaphoreType.DMA
    vm = pltpu.VMEM
    scratch = [
        vm((ROWS, depth), bf), vm((1, depth), f32), vm((seq, depth), bf), vm((depth, cols), bf),
        vm((seq, cols), bf), vm((seq, cols), bf), vm(dout.shape, bf), vm(table.shape, f32),
        vm((seq, HEAD), f32), vm((seq, HEAD), f32),
        vm((seq, depth), bf),
        vm((13 * UNIT, depth), bf), vm((13 * UNIT, depth), bf),
        vm((13 * UNIT, depth // 2), bf), vm((13 * UNIT, depth // 2), bf), vm((17 * UNIT, depth), bf),
        vm((8, 1, depth), f32), vm((8, depth), f32),
        vm((64, depth), bf), vm((32, depth), bf), vm((32, depth), f32), vm((nz, 32, zcols), f32),
        vm((32, zcols), f32), vm((16, zcols), f32), vm((nz, 32, zcols), f32), vm((nz, 32, zcols), f32),
        vm((64, depth), f32), vm((64, depth), f32),
        dma((10,)),
    ]
    scratch += [dma((n,)) for n in (26, 26, 17) * 4]
    scratch += [dma((n,)) for n in (8, 8, 4, 4, nz, nz, nz, nz)]
    operands = (tokens, gain, wq, wk, wv, dout, table, global_fragment, momentum, local_fragment)
    return pl.pallas_call(
        functools.partial(step_kernel, reps),
        out_shape=(
            jax.ShapeDtypeStruct(wq.shape, bf),
            jax.ShapeDtypeStruct(wk.shape, bf),
            jax.ShapeDtypeStruct(wv.shape, bf),
            jax.ShapeDtypeStruct((1, depth), f32),
            jax.ShapeDtypeStruct((ROWS, depth), bf),
            jax.ShapeDtypeStruct((64, depth), f32),
            jax.ShapeDtypeStruct((64, depth), f32),
        ),
        in_specs=[anywhere] * 10,
        out_specs=[pl.BlockSpec(memory_space=pltpu.VMEM)] * 7,
        scratch_shapes=scratch,
        compiler_params=pltpu.CompilerParams(
            vmem_limit_bytes=LIMIT, collective_id=0, has_side_effects=True
        ),
    )(*(pltpu.with_memory_space_constraint(a, pltpu.HBM) for a in operands))


def flush_kernel(*refs):
    count = len(refs) // 2
    sem = refs[-1]
    copies = [pltpu.make_async_copy(refs[i], refs[count + i], sem.at[i]) for i in range(count)]
    for c in copies:
        c.start()
    for c in copies:
        c.wait()


def flush(*arrays):
    return pl.pallas_call(
        flush_kernel,
        out_shape=tuple(jax.ShapeDtypeStruct(a.shape, a.dtype) for a in arrays),
        in_specs=[pl.BlockSpec(memory_space=pltpu.VMEM)] * len(arrays),
        out_specs=[pl.BlockSpec(memory_space=pl.ANY)] * len(arrays),
        scratch_shapes=[pltpu.SemaphoreType.DMA((len(arrays),))],
        compiler_params=pltpu.CompilerParams(vmem_limit_bytes=8 * 1024 * 1024),
    )(*arrays)


def body(tokens, norm_gain, w_query, key_weight, value_weight, attention_gradient, global_fragment, momentum, local_fragment):
    replicas = lax.axis_size("rep")
    gq, gk, gv, grad_gain, grad_tokens, new_global, new_momentum = run(
        replicas, tokens[0], norm_gain, w_query[0], key_weight[0], value_weight[0],
        attention_gradient[0], global_fragment, momentum, local_fragment[0],
    )
    gq, gk, gv, grad_gain, grad_tokens, new_global, new_momentum = flush(
        gq, gk, gv, grad_gain, grad_tokens, new_global, new_momentum
    )
    return (gq[None], gk[None], gv[None], grad_gain, grad_tokens[None], new_global, new_momentum)


def solution(mesh):
    placed = (
        P("rep", "tp", None), P("rep", None), P("rep", None, "tp"), P("rep", None, "tp"), P("rep", None, "tp"),
        P("rep", None, "tp"), P("tp", None), P("tp", None), P("rep", "tp", None),
    )
    outs = (P("rep", None, "tp"), P("rep", None, "tp"), P("rep", None, "tp"), P("rep", None), P("rep", "tp", None), P("tp", None), P("tp", None))
    return jax.shard_map(body, mesh=mesh, in_specs=placed, out_specs=outs, check_vma=False)
```

```python
import functools

import jax
import jax.numpy as jnp
import numpy as np
from jax import lax
from jax.experimental import pallas as pl
from jax.experimental.pallas import tpu as pltpu
from jax.sharding import PartitionSpec as P

HEAD = 128
EPSILON = 1e-05
ROPE_BASE = 500000.0
OUTER_RATE = 0.7
OUTER_MOMENTUM = 0.9
NEGATIVE = -1e30


def rope_constants(seq):
    half = HEAD // 2
    freq = ROPE_BASE ** (-2.0 * np.arange(half, dtype=np.float64) / HEAD)
    angle = np.arange(seq, dtype=np.float64)[:, None] * freq[None, :]
    cos, sin = np.cos(angle), np.sin(angle)
    table = np.concatenate([cos, cos, -sin, sin], axis=1)
    return jnp.asarray(table.astype(np.float32))


def rope(v, cos, sin):
    return v * cos + pltpu.roll(v, HEAD // 2, 1) * sin


def unrope(g, cos, sin):
    return g * cos - pltpu.roll(g, HEAD // 2, 1) * sin


def project(rows, x, weights, table, qkv):
    heads = qkv.shape[1] // HEAD
    cos = table[rows, :HEAD]
    sin = table[rows, HEAD:]
    out = jnp.dot(x, weights[...], preferred_element_type=jnp.float32)
    for h in range(heads):
        part = out[:, h * HEAD : (h + 1) * HEAD]
        if h < heads - 1:
            part = rope(part, cos, sin)
        qkv[rows, h * HEAD : (h + 1) * HEAD] = part.astype(jnp.bfloat16)


def dot_t(a, b):
    return lax.dot_general(a, b, (((1,), (1,)), ((), ())), preferred_element_type=jnp.float32)


def t_dot(a, b):
    return lax.dot_general(a, b, (((0,), (0,)), ((), ())), preferred_element_type=jnp.float32)


def attention_rows(start, block, qkv, dout, table, dqkv, acc_k, acc_v, first):
    width = start + block
    scale = HEAD ** (-0.5)
    power_scale = scale * 1.4426950408889634
    heads = dout.shape[1] // HEAD
    at_k, at_v = heads * HEAD, (heads + 1) * HEAD
    keys = qkv[:width, at_k : at_k + HEAD]
    values = qkv[:width, at_v : at_v + HEAD]
    rows = slice(start, start + block)
    key = lax.broadcasted_iota(jnp.int32, (block, block), 0)
    query = lax.broadcasted_iota(jnp.int32, (block, block), 1)
    allowed = key <= query
    cos, sin = table[rows, :HEAD], table[rows, HEAD:]
    dk = dv = None
    for h in range(heads):
        q = qkv[rows, h * HEAD : (h + 1) * HEAD]
        do = dout[rows, h * HEAD : (h + 1) * HEAD]
        s = dot_t(keys, q)
        last = jnp.where(allowed, s[start:, :], NEGATIVE)
        s = last if start == 0 else jnp.concatenate([s[:start, :], last], axis=0)
        top = jnp.max(s, axis=0, keepdims=True)
        power = jnp.exp2((s - top) * power_scale)
        inverse = 1.0 / jnp.sum(power, axis=0, keepdims=True)
        p_low = power.astype(jnp.bfloat16)
        dp = dot_t(values, do)
        drop = jnp.sum(dp * power, axis=0, keepdims=True) * inverse
        ds = (power * (dp - drop)).astype(jnp.bfloat16)
        dq = (t_dot(keys, ds) * (inverse * scale)).T
        by_row = jnp.broadcast_to(inverse, (HEAD, block)).T
        do = (do.astype(jnp.float32) * by_row).astype(jnp.bfloat16)
        q = (q.astype(jnp.float32) * (by_row * scale)).astype(jnp.bfloat16)
        dqkv[rows, h * HEAD : (h + 1) * HEAD] = unrope(dq, cos, sin).astype(jnp.bfloat16)
        tv = jnp.dot(p_low, do, preferred_element_type=jnp.float32)
        tk = jnp.dot(ds, q, preferred_element_type=jnp.float32)
        dv = tv if dv is None else dv + tv
        dk = tk if dk is None else dk + tk
    if first:
        acc_v[:width, :] = dv
        acc_k[:width, :] = dk
    else:
        acc_v[:width, :] += dv
        acc_k[:width, :] += dk
    dqkv[rows, at_k : at_k + HEAD] = unrope(acc_k[rows, :], cos, sin).astype(jnp.bfloat16)
    dqkv[rows, at_v : at_v + HEAD] = acc_v[rows, :].astype(jnp.bfloat16)


ROWS = 128
UNIT = 16
UNITS = ROWS // UNIT
BLOCK = 256
FIRST = 5
STEPS = 12
LIMIT = 44 * 1024 * 1024


def units(count, step, start=0):
    def one(i, carry):
        step(i)
        return carry

    lax.fori_loop(start, start + count, one, 0)


def normalise(rows, tokens):
    wide = tokens[rows, :].astype(jnp.float32)
    inverse = lax.rsqrt(jnp.mean(wide * wide, axis=1, keepdims=True) + EPSILON)
    return wide * inverse, inverse


def step_kernel(
    reps,
    tokens_h, gain_h, wq_h, wk_h, wv_h, dout_h, table_h, global_h, momentum_h, local_h,
    gq, gk, gv, ggain, gtok, new_global, new_momentum,
    tokens, gain, xf, weights, qkv, dqkv, dout, table, acc_k, acc_v,
    part, full_p, full_m, half_p, half_m, from_x,
    gbuf, gsum,
    frag, buf_a, acc_a, buf_c, acc_c, buf_b, mean_a, mean_o, glob, mom,
    load,
    asp, asm, asx, arp, arm, arx,
    rsp, rsm, rsx, rrp, rrm, rrx,
    gs, gr, fs, fr, fcs, fcr, fds, fdr,
):
    f32, bf = jnp.float32, jnp.bfloat16
    depth = xf.shape[1]
    mid = depth // 2
    r, t = lax.axis_index("rep"), lax.axis_index("tp")
    nz = reps // 4
    xh, z, core = r // (2 * nz), (r // 2) % nz, r % 2
    cx, y = t // 4, t % 4
    ox = 1 - cx
    up, dn, far = (y + 1) % 4, (y + 3) % 4, (y + 2) % 4

    def tp_dev(col, row):
        return (r, col * 4 + row)

    def rep_dev(h, zz, c):
        return (h * (2 * nz) + zz * 2 + c, t)

    dev_p, dev_m, dev_x = tp_dev(cx, up), tp_dev(cx, dn), tp_dev(ox, y)
    dev_core, dev_h = rep_dev(xh, z, 1 - core), rep_dev(1 - xh, z, core)

    def rdma(src, dst, s, d, dev):
        return pltpu.make_async_remote_copy(
            src_ref=src, dst_ref=dst, send_sem=s, recv_sem=d,
            device_id=dev, device_id_type=pl.DeviceIdType.MESH,
        )

    barrier = pltpu.get_barrier_semaphore()
    peers = [(r, (t + d) % 8) for d in range(1, 8)]
    peers += [dev_core, dev_h] + [rep_dev(xh, (z + d) % nz, core) for d in range(1, nz)]
    for p in peers:
        pl.semaphore_signal(barrier, inc=1, device_id=p, device_id_type=pl.DeviceIdType.MESH)

    wide_q = wq_h.shape[1]
    loads = [
        (tokens_h, tokens),
        (gain_h, gain),
        (local_h, frag),
        (wq_h, weights.at[:, :wide_q]),
        (wk_h, weights.at[:, wide_q : wide_q + HEAD]),
        (wv_h, weights.at[:, wide_q + HEAD :]),
        (table_h, table),
        (dout_h, dout),
        (global_h, glob),
        (momentum_h, mom),
    ]
    loads = [pltpu.make_async_copy(a, b, load.at[i]) for i, (a, b) in enumerate(loads)]
    for c in loads:
        c.start()
    loads[0].wait()
    loads[1].wait()

    def norm_unit(u):
        rows = pl.ds(pl.multiple_of(u * UNIT, UNIT), UNIT)
        xhat, _ = normalise(rows, tokens)
        at = pl.ds(pl.multiple_of(t * ROWS + u * UNIT, UNIT), UNIT)
        xf[at, :] = (xhat * gain[...]).astype(bf)

    units(UNITS, norm_unit)
    loads[2].wait()
    pl.semaphore_wait(barrier, len(peers))

    def frag_a():
        other = pl.ds(pl.multiple_of((1 - core) * 32, 32), 32)
        return rdma(frag.at[other, :], buf_a, fs.at[0], fr.at[0], dev_core)

    def place(ref, col, row, u, half=None):
        rows = pl.ds(pl.multiple_of((col * 4 + row) * ROWS + u * UNIT, UNIT), UNIT)
        if half is None:
            return ref.at[rows, :]
        return ref.at[rows, half * mid : (half + 1) * mid]

    def gather(way, i, col, row, u, half=None):
        s, d, dev = ((asp, arp, dev_p), (asm, arm, dev_m), (asx, arx, dev_x))[way]
        ref = place(xf, col, row, u, half)
        return rdma(ref, ref, s.at[i], d.at[i], dev)

    def send_own(i):
        u = (i + FIRST) % UNITS
        for way in range(3):
            gather(way, u, cx, y, u).start()

    units(UNITS, send_own)
    frag_a().start()
    gsum[...] = jnp.zeros_like(gsum)
    for c in loads[3:]:
        c.wait()

    later = UNITS - FIRST

    def relay_later(i):
        u = FIRST + i
        gather(0, u, cx, dn, u).wait_recv()
        gather(0, 13 + u, cx, dn, u, 0).start()
        gather(2, 8 + i, cx, dn, u).start()
        gather(1, u, cx, up, u).wait_recv()
        gather(1, 13 + u, cx, up, u, 1).start()
        gather(2, 11 + i, cx, up, u).start()

    def relay_first(u):
        gather(0, u, cx, dn, u).wait_recv()
        gather(0, 13 + u, cx, dn, u, 0).start()
        gather(1, u, cx, up, u).wait_recv()
        gather(1, 13 + u, cx, up, u, 1).start()
        gather(2, u, ox, y, u).wait_recv()
        gather(0, 8 + u, ox, y, u).start()
        gather(1, 8 + u, ox, y, u).start()

    def relay_far(i):
        u = FIRST + i
        gather(0, 13 + u, cx, far, u, 0).wait_recv()
        gather(1, 13 + u, cx, far, u, 1).wait_recv()
        gather(2, 14 + i, cx, far, u).start()

    def relay_other(u):
        gather(0, 8 + u, ox, dn, u).wait_recv()
        gather(0, 21 + u, ox, dn, u, 0).start()
        gather(1, 8 + u, ox, up, u).wait_recv()
        gather(1, 21 + u, ox, up, u, 1).start()

    zcols = depth // nz

    def frag_c(d):
        peer = (z + d) % nz
        return rdma(
            acc_a.at[:, pl.ds(pl.multiple_of(peer * zcols, 128), zcols)], buf_c.at[z],
            fcs.at[d], fcr.at[d], rep_dev(xh, peer, core),
        )

    def frag_b():
        other = pl.ds(pl.multiple_of((1 - xh) * 16, 16), 16)
        return rdma(acc_c.at[other, :], buf_b, fs.at[1], fr.at[1], dev_h)

    def frag_b_back():
        mine = mean_a.at[z, pl.ds(pl.multiple_of(xh * 16, 16), 16), :]
        return rdma(mine, mine, fs.at[2], fr.at[2], dev_h)

    def frag_c_back(d):
        return rdma(mean_a.at[z], mean_a.at[z], fds.at[d], fdr.at[d], rep_dev(xh, (z + d) % nz, core))

    def frag_a_back():
        return rdma(mean_a, mean_o, fs.at[3], fr.at[3], dev_core)

    def frag_step(k):
        if k == 0:
            frag_a().wait_recv()
            own = frag[pl.ds(pl.multiple_of(core * 32, 32), 32), :]
            acc_a[...] = own.astype(f32) + buf_a[...].astype(f32)
        elif k == 1:
            for d in range(1, nz):
                frag_c(d).start()
        elif k == 2:
            for d in range(1, nz):
                frag_c(d).wait_recv()
            total = acc_a[:, pl.ds(pl.multiple_of(z * zcols, 128), zcols)]
            for d in range(1, nz):
                total += buf_c[(z + d) % nz]
            acc_c[...] = total
        elif k == 3:
            frag_b().start()
        elif k == 4:
            frag_b().wait_recv()
            rows = pl.ds(pl.multiple_of(xh * 16, 16), 16)
            mean_a[z, rows, :] = (
                glob[
                    pl.ds(pl.multiple_of(core * 32 + xh * 16, 16), 16),
                    pl.ds(pl.multiple_of(z * zcols, 128), zcols),
                ]
                - (acc_c[rows, :] + buf_b[...]) * (1.0 / reps)
            )
        elif k == 5:
            frag_b_back().start()
        elif k == 6:
            other = mean_a.at[z, pl.ds(pl.multiple_of((1 - xh) * 16, 16), 16), :]
            rdma(other, other, fs.at[2], fr.at[2], dev_h).wait_recv()
            for d in range(1, nz):
                frag_c_back(d).start()
        elif k == 7:
            for d in range(1, nz):
                slot = mean_a.at[(z + nz - d) % nz]
                rdma(slot, slot, fds.at[d], fdr.at[d], rep_dev(xh, (z + d) % nz, core)).wait_recv()
            frag_a_back().start()
        elif k == 8:
            frag_a_back().wait_recv()

    def outer_update(zz):
        cols = slice(zz * zcols, (zz + 1) * zcols)
        for which, src in ((core, mean_a), (1 - core, mean_o)):
            rows = pl.ds(pl.multiple_of(which * 32, 32), 32)
            mean = src[zz]
            moved = OUTER_MOMENTUM * mom[rows, cols] + mean
            new_momentum[rows, cols] = moved
            new_global[rows, cols] = glob[rows, cols] - OUTER_RATE * (mean + OUTER_MOMENTUM * moved)

    def gather_stage(s):
        @pl.when(s == 0)
        def _():
            frag_step(0)

        @pl.when(s == 1)
        def _():
            frag_step(1)
            units(later, relay_later)
            units(FIRST, relay_first)
            units(later, lambda i: gather(2, FIRST + i, ox, y, FIRST + i).wait_recv())

        @pl.when(s == 2)
        def _():
            frag_step(2)

        @pl.when(s == 3)
        def _():
            frag_step(3)

        @pl.when(s == 4)
        def _():
            units(later, relay_far)
            frag_step(4)
            units(FIRST, relay_other)
            frag_step(5)

            def landed(u):
                gather(0, 13 + u, cx, far, u, 0).wait_recv()
                gather(1, 13 + u, cx, far, u, 1).wait_recv()

            units(FIRST, landed)

        @pl.when(s == 5)
        def _():
            frag_step(6)
            units(later, lambda i: gather(2, 8 + i, ox, dn, FIRST + i).wait_recv())

        @pl.when(s == 6)
        def _():
            units(later, lambda i: gather(2, 11 + i, ox, up, FIRST + i).wait_recv())

        @pl.when(s == 7)
        def _():
            def landed(u):
                gather(0, 21 + u, ox, far, u, 0).wait_recv()
                gather(1, 21 + u, ox, far, u, 1).wait_recv()

            units(FIRST, landed)
            units(later, lambda i: gather(2, 14 + i, ox, far, FIRST + i).wait_recv())

        k = (s + 1) % 3
        d = 3 - 2 * k + 3 * (k * (k - 1) // 2)
        beyond = (s + 6) // 8
        row = (y + d * beyond) % 4
        other = (1 - beyond) * (s % 2) + beyond * ((s + 3) // 8)
        col = cx + other * (1 - 2 * cx)
        at = pl.ds(pl.multiple_of((col * 4 + row) * ROWS, ROWS), ROWS)
        project(at, xf[at, :], weights, table, qkv)

    units(8, gather_stage)

    def scatter(way, i, src, dst):
        s, d, dev = ((rsp, rrp, dev_p), (rsm, rrm, dev_m), (rsx, rrx, dev_x))[way]
        return rdma(src, dst, s.at[i], d.at[i], dev)

    def slot(ref, i):
        return ref.at[pl.ds(pl.multiple_of(i * UNIT, UNIT), UNIT), :]

    def scatter_full(way, i, col, row, u):
        return scatter(way, i, place(part, col, row, u), slot((full_p, full_m)[way], i))

    def scatter_half(way, i, col, row, u):
        half = 1 - way
        return scatter(way, 13 + i, place(part, col, row, u, half), slot((half_p, half_m)[way], i))

    def scatter_x(i, col, row, u):
        return scatter(2, i, place(part, col, row, u), slot(from_x, i))

    def add(col, row, u, terms, half=None):
        rows = pl.ds(pl.multiple_of((col * 4 + row) * ROWS + u * UNIT, UNIT), UNIT)
        cols = slice(0, depth) if half is None else slice(half * mid, (half + 1) * mid)
        total = part[rows, cols].astype(f32)
        for ref, i in terms:
            total += ref[pl.ds(pl.multiple_of(i * UNIT, UNIT), UNIT), :].astype(f32)
        part[rows, cols] = total.astype(bf)

    def near(i, col, u):
        scatter_half(0, i, col, far, u).wait_recv()
        add(col, up, u, [(half_p, i)], 1)
        scatter_half(1, i, col, far, u).wait_recv()
        add(col, dn, u, [(half_m, i)], 0)
        scatter_full(0, i, col, up, u).start()
        scatter_full(1, i, col, dn, u).start()

    def across(i):
        scatter_full(0, i, ox, y, i).wait_recv()
        scatter_full(1, i, ox, y, i).wait_recv()
        add(ox, y, i, [(full_p, i), (full_m, i)])
        scatter_x(12 + i, ox, y, i).start()

    def far_halves(i, col, u):
        scatter_half(0, i, col, far, u).start()
        scatter_half(1, i, col, far, u).start()

    def far_later(i):
        u = FIRST + i
        scatter_x(3 + i, cx, far, u).wait_recv()
        add(cx, far, u, [(from_x, 3 + i)])
        far_halves(5 + u, cx, u)

    def side_later(i):
        u = FIRST + i
        scatter_x(i, cx, up, u).wait_recv()
        add(cx, up, u, [(from_x, i)])
        scatter_x(6 + i, cx, dn, u).wait_recv()
        add(cx, dn, u, [(from_x, 6 + i)])

    def terms(chunk):
        col, row = chunk // 4, chunk % 4
        away = (row + 4 - y) % 4
        other = (col + cx) % 2
        at = pl.ds(pl.multiple_of(chunk * ROWS, ROWS), ROWS)
        width = min(512, depth)
        for j in range(0, depth, width):
            cols = slice(j, j + width)
            low = dot_t(dqkv[at, :], weights[cols, :]).astype(bf)
            part[at, cols] = low
            moved = low.astype(f32) * xf[at, cols].astype(f32)
            gsum[:, cols] += jnp.sum(moved.reshape(ROWS // 8, 8, width), axis=0)

        @pl.when(other == 1)
        def _():
            role = (away + 3) % 4
            units(later, lambda i: scatter_x(3 * role + i, ox, row, FIRST + i).start())

        @pl.when(away == 2)
        def _():
            units(FIRST, lambda u: far_halves(5 * (1 - other) + u, col, u))

    def after_3(i):
        terms(6 + (far + i) % 2)

    def after_2(i):
        terms((1 - cx) * (4 + (far + i) % 2) + cx * (4 + far))

    def after_1(i):
        terms(2 + (far + i) % 2)

    def after_0(i):
        own = 1 - cx * (1 - (i + 2) // 4)
        k = (i - cx) * own
        d = 2 - k + 3 * (k // 2) - 2 * (k // 3)
        terms(own * (cx * 4 + (y + d) % 4) + (1 - own) * ((far + i) % 2))

        @pl.when(i == 1 + 3 * cx)
        def _():
            units(FIRST, lambda u: near(u, ox, u))

    seq = qkv.shape[0]
    after = ((after_0, 4 + cx), (after_1, 2 * cx), (after_2, 2 - cx), (after_3, 2 * (1 - cx)))
    for b in reversed(range(4)):
        start = b * BLOCK
        attention_rows(start, BLOCK, qkv, dout, table, dqkv, acc_k, acc_v, start + BLOCK == seq)
        units(after[b][1], after[b][0])

    gbuf[t] = jnp.sum(gsum[...], axis=0, keepdims=True)
    def gain_to(d):
        return rdma(gbuf.at[t], gbuf.at[t], gs.at[d], gr.at[d], (r, (t + d) % 8))

    for d in range(1, 8):
        gain_to(d).start()
    frag_step(7)

    def early_sends_ended():
        units(8, lambda i: [gather(w, i, cx, y, i).wait_send() for w in range(3)] and None)
        units(FIRST, lambda i: [gather(w, 8 + i, ox, y, i).wait_send() for w in range(2)] and None)
        units(13, lambda i: [gather(w, 13 + i, cx, y, 0, w).wait_send() for w in range(2)] and None)
        units(9, lambda i: gather(2, 8 + i, cx, y, 0).wait_send())
        for d in range(1, 8):
            gain_to(d).wait_send()
        for d in range(1, nz):
            frag_c(d).wait_send()
            frag_c_back(d).wait_send()
        frag_a().wait_send()
        frag_b().wait_send()
        frag_b_back().wait_send()
        frag_a_back().wait_send()

    def most_sends_ended():
        units(13, lambda i: [scatter_half(w, i, cx, y, 0).wait_send() for w in range(2)] and None)
        units(5 + FIRST, lambda i: [scatter_full(w, i, cx, y, 0).wait_send() for w in range(2)] and None)
        units(12, lambda i: scatter_x(i, cx, y, 0).wait_send())

    def weight_stage(j):
        @pl.when(j == 0)
        def _():
            units(3, lambda u: near(5 + u, cx, u))

        @pl.when(j == 3)
        def _():
            units(FIRST, across)

        @pl.when(j == 5)
        def _():
            units(later, far_later)
            units(FIRST - 3, lambda u: near(5 + u, cx, u), 3)

        @pl.when(j == 7)
        def _():
            units(later, side_later)

        @pl.when(j == 8)
        def _():
            units(later, lambda i: near(5 + FIRST + i, cx, FIRST + i))

        @pl.when(j == 9)
        def _():
            frag_step(8)
            for zz in range(nz):
                outer_update(zz)

        @pl.when(j == 10)
        def _():
            for d in range(1, 8):
                ref = gbuf.at[(t + 8 - d) % 8]
                rdma(ref, ref, gs.at[d], gr.at[d], (r, (t + d) % 8)).wait_recv()
            total = gbuf[0]
            for d in range(1, 8):
                total += gbuf[d]
            ggain[...] = total / gain[...]
            early_sends_ended()

        block = depth // STEPS
        at = pl.ds(pl.multiple_of(j * block, block), block)
        g = t_dot(xf[:, at], dqkv[...]).astype(bf)
        gq[at, :] = g[:, :wide_q]
        gk[at, :] = g[:, wide_q : wide_q + HEAD]
        gv[at, :] = g[:, wide_q + HEAD :]

    units(STEPS, weight_stage)
    most_sends_ended()

    def finish(u):
        @pl.when(u < FIRST)
        def _():
            scatter_x(12 + u, cx, y, u).wait_recv()

        @pl.when(u >= FIRST)
        def _():
            scatter_x(9 + u - FIRST, cx, y, u).wait_recv()

        at_x = (12 + u) * (1 - u // FIRST) + (4 + u) * (u // FIRST)
        scatter_full(0, 5 + u, cx, y, u).wait_recv()
        scatter_full(1, 5 + u, cx, y, u).wait_recv()

        def term(ref, i):
            return ref[pl.ds(pl.multiple_of(i * UNIT, UNIT), UNIT), :].astype(f32)

        mine = (cx * 4 + y) * UNITS + u
        total = (term(part, mine) + term(from_x, at_x)) + (term(full_p, 5 + u) + term(full_m, 5 + u))
        rows = pl.ds(pl.multiple_of(u * UNIT, UNIT), UNIT)
        xhat, inverse = normalise(rows, tokens)
        scaled = total * gain[...]
        mean = jnp.mean(scaled * xhat, axis=1, keepdims=True)
        gtok[rows, :] = (inverse * (scaled - xhat * mean)).astype(bf)

    units(UNITS, finish)

    units(later, lambda i: [scatter_full(w, 5 + FIRST + i, cx, y, 0).wait_send() for w in range(2)] and None)
    units(FIRST, lambda i: scatter_x(12 + i, cx, y, 0).wait_send())


def run(reps, tokens, gain, wq, wk, wv, dout, global_fragment, momentum, local_fragment):
    depth = tokens.shape[1]
    seq = dout.shape[0]
    table = rope_constants(seq)
    f32, bf = jnp.float32, jnp.bfloat16
    cols = wq.shape[1] + wk.shape[1] + wv.shape[1]
    anywhere = pl.BlockSpec(memory_space=pltpu.HBM)
    nz = reps // 4
    zcols = depth // nz
    dma = pltpu.SemaphoreType.DMA
    vm = pltpu.VMEM
    scratch = [
        vm((ROWS, depth), bf), vm((1, depth), f32), vm((seq, depth), bf), vm((depth, cols), bf),
        vm((seq, cols), bf), vm((seq, cols), bf), vm(dout.shape, bf), vm(table.shape, f32),
        vm((seq, HEAD), f32), vm((seq, HEAD), f32),
        vm((seq, depth), bf),
        vm((13 * UNIT, depth), bf), vm((13 * UNIT, depth), bf),
        vm((13 * UNIT, depth // 2), bf), vm((13 * UNIT, depth // 2), bf), vm((17 * UNIT, depth), bf),
        vm((8, 1, depth), f32), vm((8, depth), f32),
        vm((64, depth), bf), vm((32, depth), bf), vm((32, depth), f32), vm((nz, 32, zcols), f32),
        vm((32, zcols), f32), vm((16, zcols), f32), vm((nz, 32, zcols), f32), vm((nz, 32, zcols), f32),
        vm((64, depth), f32), vm((64, depth), f32),
        dma((10,)),
    ]
    scratch += [dma((n,)) for n in (26, 26, 17) * 4]
    scratch += [dma((n,)) for n in (8, 8, 4, 4, nz, nz, nz, nz)]
    operands = (tokens, gain, wq, wk, wv, dout, table, global_fragment, momentum, local_fragment)
    return pl.pallas_call(
        functools.partial(step_kernel, reps),
        out_shape=(
            jax.ShapeDtypeStruct(wq.shape, bf),
            jax.ShapeDtypeStruct(wk.shape, bf),
            jax.ShapeDtypeStruct(wv.shape, bf),
            jax.ShapeDtypeStruct((1, depth), f32),
            jax.ShapeDtypeStruct((ROWS, depth), bf),
            jax.ShapeDtypeStruct((64, depth), f32),
            jax.ShapeDtypeStruct((64, depth), f32),
        ),
        in_specs=[anywhere] * 10,
        out_specs=[pl.BlockSpec(memory_space=pltpu.VMEM)] * 7,
        scratch_shapes=scratch,
        compiler_params=pltpu.CompilerParams(
            vmem_limit_bytes=LIMIT, collective_id=0, has_side_effects=True
        ),
    )(*(pltpu.with_memory_space_constraint(a, pltpu.HBM) for a in operands))


def flush_kernel(*refs):
    count = len(refs) // 2
    sem = refs[-1]
    copies = [pltpu.make_async_copy(refs[i], refs[count + i], sem.at[i]) for i in range(count)]
    for c in copies:
        c.start()
    for c in copies:
        c.wait()


def flush(*arrays):
    return pl.pallas_call(
        flush_kernel,
        out_shape=tuple(jax.ShapeDtypeStruct(a.shape, a.dtype) for a in arrays),
        in_specs=[pl.BlockSpec(memory_space=pltpu.VMEM)] * len(arrays),
        out_specs=[pl.BlockSpec(memory_space=pl.ANY)] * len(arrays),
        scratch_shapes=[pltpu.SemaphoreType.DMA((len(arrays),))],
        compiler_params=pltpu.CompilerParams(vmem_limit_bytes=8 * 1024 * 1024),
    )(*arrays)


def body(tokens, norm_gain, w_query, key_weight, value_weight, attention_gradient, global_fragment, momentum, local_fragment):
    replicas = lax.axis_size("rep")
    gq, gk, gv, grad_gain, grad_tokens, new_global, new_momentum = run(
        replicas, tokens[0], norm_gain, w_query[0], key_weight[0], value_weight[0],
        attention_gradient[0], global_fragment, momentum, local_fragment[0],
    )
    gq, gk, gv, grad_gain, grad_tokens, new_global, new_momentum = flush(
        gq, gk, gv, grad_gain, grad_tokens, new_global, new_momentum
    )
    return (gq[None], gk[None], gv[None], grad_gain, grad_tokens[None], new_global, new_momentum)


def solution(mesh):
    placed = (
        P("rep", "tp", None), P("rep", None), P("rep", None, "tp"), P("rep", None, "tp"), P("rep", None, "tp"),
        P("rep", None, "tp"), P("tp", None), P("tp", None), P("rep", "tp", None),
    )
    outs = (P("rep", None, "tp"), P("rep", None, "tp"), P("rep", None, "tp"), P("rep", None), P("rep", "tp", None), P("tp", None), P("tp", None))
    return jax.shard_map(body, mesh=mesh, in_specs=placed, out_specs=outs, check_vma=False)
```

```python
import functools

import jax
import jax.numpy as jnp
import numpy as np
from jax import lax
from jax.experimental import pallas as pl
from jax.experimental.pallas import tpu as pltpu
from jax.sharding import PartitionSpec as P

HEAD = 128
EPSILON = 1e-05
ROPE_BASE = 500000.0
OUTER_RATE = 0.7
OUTER_MOMENTUM = 0.9
NEGATIVE = -1e30


def rope_constants(seq):
    half = HEAD // 2
    freq = ROPE_BASE ** (-2.0 * np.arange(half, dtype=np.float64) / HEAD)
    angle = np.arange(seq, dtype=np.float64)[:, None] * freq[None, :]
    cos, sin = np.cos(angle), np.sin(angle)
    table = np.concatenate([cos, cos, -sin, sin], axis=1)
    return jnp.asarray(table.astype(np.float32))


def rope(v, cos, sin):
    return v * cos + pltpu.roll(v, HEAD // 2, 1) * sin


def unrope(g, cos, sin):
    return g * cos - pltpu.roll(g, HEAD // 2, 1) * sin


def project(rows, x, weights, table, qkv):
    heads = qkv.shape[1] // HEAD
    cos = table[rows, :HEAD]
    sin = table[rows, HEAD:]
    out = jnp.dot(x, weights[...], preferred_element_type=jnp.float32)
    for h in range(heads):
        part = out[:, h * HEAD : (h + 1) * HEAD]
        if h < heads - 1:
            part = rope(part, cos, sin)
        qkv[rows, h * HEAD : (h + 1) * HEAD] = part.astype(jnp.bfloat16)


def dot_t(a, b):
    return lax.dot_general(a, b, (((1,), (1,)), ((), ())), preferred_element_type=jnp.float32)


def t_dot(a, b):
    return lax.dot_general(a, b, (((0,), (0,)), ((), ())), preferred_element_type=jnp.float32)


def attention_rows(start, block, qkv, dout, table, dqkv, acc_k, acc_v, first):
    width = start + block
    scale = HEAD ** (-0.5)
    power_scale = scale * 1.4426950408889634
    heads = dout.shape[1] // HEAD
    at_k, at_v = heads * HEAD, (heads + 1) * HEAD
    keys = qkv[:width, at_k : at_k + HEAD]
    values = qkv[:width, at_v : at_v + HEAD]
    rows = slice(start, start + block)
    key = lax.broadcasted_iota(jnp.int32, (block, block), 0)
    query = lax.broadcasted_iota(jnp.int32, (block, block), 1)
    allowed = key <= query
    cos, sin = table[rows, :HEAD], table[rows, HEAD:]
    dk = dv = None
    for h in range(heads):
        q = qkv[rows, h * HEAD : (h + 1) * HEAD]
        do = dout[rows, h * HEAD : (h + 1) * HEAD]
        s = dot_t(keys, q)
        last = jnp.where(allowed, s[start:, :], NEGATIVE)
        s = last if start == 0 else jnp.concatenate([s[:start, :], last], axis=0)
        top = jnp.max(s, axis=0, keepdims=True)
        power = jnp.exp2((s - top) * power_scale)
        inverse = 1.0 / jnp.sum(power, axis=0, keepdims=True)
        p_low = power.astype(jnp.bfloat16)
        dp = dot_t(values, do)
        drop = jnp.sum(dp * power, axis=0, keepdims=True) * inverse
        ds = (power * (dp - drop)).astype(jnp.bfloat16)
        dq = (t_dot(keys, ds) * (inverse * scale)).T
        by_row = jnp.broadcast_to(inverse, (HEAD, block)).T
        do = (do.astype(jnp.float32) * by_row).astype(jnp.bfloat16)
        q = (q.astype(jnp.float32) * (by_row * scale)).astype(jnp.bfloat16)
        dqkv[rows, h * HEAD : (h + 1) * HEAD] = unrope(dq, cos, sin).astype(jnp.bfloat16)
        tv = jnp.dot(p_low, do, preferred_element_type=jnp.float32)
        tk = jnp.dot(ds, q, preferred_element_type=jnp.float32)
        dv = tv if dv is None else dv + tv
        dk = tk if dk is None else dk + tk
    if first:
        acc_v[:width, :] = dv
        acc_k[:width, :] = dk
    else:
        acc_v[:width, :] += dv
        acc_k[:width, :] += dk
    dqkv[rows, at_k : at_k + HEAD] = unrope(acc_k[rows, :], cos, sin).astype(jnp.bfloat16)
    dqkv[rows, at_v : at_v + HEAD] = acc_v[rows, :].astype(jnp.bfloat16)


ROWS = 128
UNIT = 16
UNITS = ROWS // UNIT
BLOCK = 256
FIRST = 5
STEPS = 12
PIECES = 4
LIMIT = 44 * 1024 * 1024


def units(count, step, start=0):
    def one(i, carry):
        step(i)
        return carry

    lax.fori_loop(start, start + count, one, 0)


def normalise(rows, tokens):
    wide = tokens[rows, :].astype(jnp.float32)
    inverse = lax.rsqrt(jnp.mean(wide * wide, axis=1, keepdims=True) + EPSILON)
    return wide * inverse, inverse


def step_kernel(
    reps,
    tokens_h, gain_h, wq_h, wk_h, wv_h, dout_h, table_h, global_h, momentum_h, local_h,
    gq, gk, gv, ggain, gtok, new_global, new_momentum,
    tokens, gain, xf, weights, qkv, dqkv, dout, table, acc_k, acc_v,
    part, full_p, full_m, half_p, half_m, from_x,
    gbuf, gsum,
    frag, buf_a, acc_a, buf_c, acc_c, buf_b, mean_a, mean_o, glob, mom,
    load,
    asp, asm, asx, arp, arm, arx,
    rsp, rsm, rsx, rrp, rrm, rrx,
    gs, gr, fs, fr, fcs, fcr, fds, fdr,
):
    f32, bf = jnp.float32, jnp.bfloat16
    depth = xf.shape[1]
    mid = depth // 2
    r, t = lax.axis_index("rep"), lax.axis_index("tp")
    nz = reps // 4
    xh, z, core = r // (2 * nz), (r // 2) % nz, r % 2
    cx, y = t // 4, t % 4
    ox = 1 - cx
    up, dn, far = (y + 1) % 4, (y + 3) % 4, (y + 2) % 4

    def tp_dev(col, row):
        return (r, col * 4 + row)

    def rep_dev(h, zz, c):
        return (h * (2 * nz) + zz * 2 + c, t)

    dev_p, dev_m, dev_x = tp_dev(cx, up), tp_dev(cx, dn), tp_dev(ox, y)
    dev_core, dev_h = rep_dev(xh, z, 1 - core), rep_dev(1 - xh, z, core)

    def rdma(src, dst, s, d, dev):
        return pltpu.make_async_remote_copy(
            src_ref=src, dst_ref=dst, send_sem=s, recv_sem=d,
            device_id=dev, device_id_type=pl.DeviceIdType.MESH,
        )

    barrier = pltpu.get_barrier_semaphore()
    peers = [(r, (t + d) % 8) for d in range(1, 8)]
    peers += [dev_core, dev_h] + [rep_dev(xh, (z + d) % nz, core) for d in range(1, nz)]
    for p in reversed(peers):
        pl.semaphore_signal(barrier, inc=1, device_id=p, device_id_type=pl.DeviceIdType.MESH)

    wide_q = wq_h.shape[1]
    loads = [
        (tokens_h, tokens),
        (gain_h, gain),
        (local_h, frag),
        (wq_h, weights.at[:, :wide_q]),
        (wk_h, weights.at[:, wide_q : wide_q + HEAD]),
        (wv_h, weights.at[:, wide_q + HEAD :]),
        (table_h, table),
        (dout_h, dout),
        (global_h, glob),
        (momentum_h, mom),
    ]
    loads = [pltpu.make_async_copy(a, b, load.at[i]) for i, (a, b) in enumerate(loads)]
    for c in loads:
        c.start()
    loads[0].wait()
    loads[1].wait()

    def norm_unit(u):
        rows = pl.ds(pl.multiple_of(u * UNIT, UNIT), UNIT)
        xhat, _ = normalise(rows, tokens)
        at = pl.ds(pl.multiple_of(t * ROWS + u * UNIT, UNIT), UNIT)
        xf[at, :] = (xhat * gain[...]).astype(bf)

    units(UNITS, norm_unit)
    loads[2].wait()
    pl.semaphore_wait(barrier, len(peers))

    def frag_a():
        other = pl.ds(pl.multiple_of((1 - core) * 32, 32), 32)
        return rdma(frag.at[other, :], buf_a, fs.at[0], fr.at[0], dev_core)

    def place(ref, col, row, u, half=None):
        rows = pl.ds(pl.multiple_of((col * 4 + row) * ROWS + u * UNIT, UNIT), UNIT)
        if half is None:
            return ref.at[rows, :]
        return ref.at[rows, half * mid : (half + 1) * mid]

    def gather(way, i, col, row, u, half=None):
        s, d, dev = ((asp, arp, dev_p), (asm, arm, dev_m), (asx, arx, dev_x))[way]
        ref = place(xf, col, row, u, half)
        return rdma(ref, ref, s.at[i], d.at[i], dev)

    def send_own(i):
        u = (i + FIRST) % UNITS
        for way in range(3):
            gather(way, u, cx, y, u).start()

    units(UNITS, send_own)
    frag_a().start()
    gsum[...] = jnp.zeros_like(gsum)
    for c in loads[3:]:
        c.wait()

    later = UNITS - FIRST

    def relay_later(i):
        u = FIRST + i
        gather(0, u, cx, dn, u).wait_recv()
        gather(0, 13 + u, cx, dn, u, 0).start()
        gather(2, 8 + i, cx, dn, u).start()
        gather(1, u, cx, up, u).wait_recv()
        gather(1, 13 + u, cx, up, u, 1).start()
        gather(2, 11 + i, cx, up, u).start()

    def relay_first(u):
        gather(0, u, cx, dn, u).wait_recv()
        gather(0, 13 + u, cx, dn, u, 0).start()
        gather(1, u, cx, up, u).wait_recv()
        gather(1, 13 + u, cx, up, u, 1).start()
        gather(2, u, ox, y, u).wait_recv()
        gather(0, 8 + u, ox, y, u).start()
        gather(1, 8 + u, ox, y, u).start()

    def relay_far(i):
        u = FIRST + i
        gather(0, 13 + u, cx, far, u, 0).wait_recv()
        gather(1, 13 + u, cx, far, u, 1).wait_recv()
        gather(2, 14 + i, cx, far, u).start()

    def relay_other(u):
        gather(0, 8 + u, ox, dn, u).wait_recv()
        gather(0, 21 + u, ox, dn, u, 0).start()
        gather(1, 8 + u, ox, up, u).wait_recv()
        gather(1, 21 + u, ox, up, u, 1).start()

    zcols = depth // nz

    def frag_c(d):
        peer = (z + d) % nz
        return rdma(
            acc_a.at[:, pl.ds(pl.multiple_of(peer * zcols, 128), zcols)], buf_c.at[z],
            fcs.at[d], fcr.at[d], rep_dev(xh, peer, core),
        )

    def frag_b():
        other = pl.ds(pl.multiple_of((1 - xh) * 16, 16), 16)
        return rdma(acc_c.at[other, :], buf_b, fs.at[1], fr.at[1], dev_h)

    def frag_b_back():
        mine = mean_a.at[z, pl.ds(pl.multiple_of(xh * 16, 16), 16), :]
        return rdma(mine, mine, fs.at[2], fr.at[2], dev_h)

    def frag_c_back(d):
        return rdma(mean_a.at[z], mean_a.at[z], fds.at[d], fdr.at[d], rep_dev(xh, (z + d) % nz, core))

    def frag_a_back():
        return rdma(mean_a, mean_o, fs.at[3], fr.at[3], dev_core)

    def frag_step(k):
        if k == 0:
            frag_a().wait_recv()
            own = frag[pl.ds(pl.multiple_of(core * 32, 32), 32), :]
            acc_a[...] = own.astype(f32) + buf_a[...].astype(f32)
        elif k == 1:
            for d in range(1, nz):
                frag_c(d).start()
        elif k == 2:
            for d in range(1, nz):
                frag_c(d).wait_recv()
            total = acc_a[:, pl.ds(pl.multiple_of(z * zcols, 128), zcols)]
            for d in range(1, nz):
                total += buf_c[(z + d) % nz]
            acc_c[...] = total
        elif k == 3:
            frag_b().start()
        elif k == 4:
            frag_b().wait_recv()
            rows = pl.ds(pl.multiple_of(xh * 16, 16), 16)
            mean_a[z, rows, :] = (
                glob[
                    pl.ds(pl.multiple_of(core * 32 + xh * 16, 16), 16),
                    pl.ds(pl.multiple_of(z * zcols, 128), zcols),
                ]
                - (acc_c[rows, :] + buf_b[...]) * (1.0 / reps)
            )
        elif k == 5:
            frag_b_back().start()
        elif k == 6:
            other = mean_a.at[z, pl.ds(pl.multiple_of((1 - xh) * 16, 16), 16), :]
            rdma(other, other, fs.at[2], fr.at[2], dev_h).wait_recv()
            for d in range(1, nz):
                frag_c_back(d).start()
        elif k == 7:
            for d in range(1, nz):
                slot = mean_a.at[(z + nz - d) % nz]
                rdma(slot, slot, fds.at[d], fdr.at[d], rep_dev(xh, (z + d) % nz, core)).wait_recv()
            frag_a_back().start()
        elif k == 8:
            frag_a_back().wait_recv()

    def outer_update(zz):
        cols = slice(zz * zcols, (zz + 1) * zcols)
        for which, src in ((core, mean_a), (1 - core, mean_o)):
            rows = pl.ds(pl.multiple_of(which * 32, 32), 32)
            mean = src[zz]
            moved = OUTER_MOMENTUM * mom[rows, cols] + mean
            new_momentum[rows, cols] = moved
            new_global[rows, cols] = glob[rows, cols] - OUTER_RATE * (mean + OUTER_MOMENTUM * moved)

    def gather_stage(s):
        @pl.when(s == 0)
        def _():
            frag_step(0)

        @pl.when(s == 1)
        def _():
            frag_step(1)
            units(later, relay_later)
            units(FIRST, relay_first)
            units(later, lambda i: gather(2, FIRST + i, ox, y, FIRST + i).wait_recv())

        @pl.when(s == 2)
        def _():
            frag_step(2)

        @pl.when(s == 3)
        def _():
            frag_step(3)

        @pl.when(s == 4)
        def _():
            units(later, relay_far)
            frag_step(4)
            units(FIRST, relay_other)
            frag_step(5)

            def landed(u):
                gather(0, 13 + u, cx, far, u, 0).wait_recv()
                gather(1, 13 + u, cx, far, u, 1).wait_recv()

            units(FIRST, landed)

        @pl.when(s == 5)
        def _():
            frag_step(6)
            units(later, lambda i: gather(2, 8 + i, ox, dn, FIRST + i).wait_recv())

        @pl.when(s == 6)
        def _():
            units(later, lambda i: gather(2, 11 + i, ox, up, FIRST + i).wait_recv())

        @pl.when(s == 7)
        def _():
            def landed(u):
                gather(0, 21 + u, ox, far, u, 0).wait_recv()
                gather(1, 21 + u, ox, far, u, 1).wait_recv()

            units(FIRST, landed)
            units(later, lambda i: gather(2, 14 + i, ox, far, FIRST + i).wait_recv())

        k = (s + 1) % 3
        d = 3 - 2 * k + 3 * (k * (k - 1) // 2)
        beyond = (s + 6) // 8
        row = (y + d * beyond) % 4
        other = (1 - beyond) * (s % 2) + beyond * ((s + 3) // 8)
        col = cx + other * (1 - 2 * cx)
        at = pl.ds(pl.multiple_of((col * 4 + row) * ROWS, ROWS), ROWS)
        project(at, xf[at, :], weights, table, qkv)

    units(8, gather_stage)

    def scatter(way, i, src, dst):
        s, d, dev = ((rsp, rrp, dev_p), (rsm, rrm, dev_m), (rsx, rrx, dev_x))[way]
        return rdma(src, dst, s.at[i], d.at[i], dev)

    def slot(ref, i):
        return ref.at[pl.ds(pl.multiple_of(i * UNIT, UNIT), UNIT), :]

    def scatter_full(way, i, col, row, u):
        return scatter(way, i, place(part, col, row, u), slot((full_p, full_m)[way], i))

    def scatter_half(way, i, col, row, u):
        half = 1 - way
        return scatter(way, 13 + i, place(part, col, row, u, half), slot((half_p, half_m)[way], i))

    def scatter_x(i, col, row, u):
        return scatter(2, i, place(part, col, row, u), slot(from_x, i))

    def add(col, row, u, terms, half=None):
        rows = pl.ds(pl.multiple_of((col * 4 + row) * ROWS + u * UNIT, UNIT), UNIT)
        cols = slice(0, depth) if half is None else slice(half * mid, (half + 1) * mid)
        total = part[rows, cols].astype(f32)
        for ref, i in terms:
            total += ref[pl.ds(pl.multiple_of(i * UNIT, UNIT), UNIT), :].astype(f32)
        part[rows, cols] = total.astype(bf)

    def near(i, col, u):
        scatter_half(0, i, col, far, u).wait_recv()
        add(col, up, u, [(half_p, i)], 1)
        scatter_half(1, i, col, far, u).wait_recv()
        add(col, dn, u, [(half_m, i)], 0)
        scatter_full(0, i, col, up, u).start()
        scatter_full(1, i, col, dn, u).start()

    def across(i):
        scatter_full(0, i, ox, y, i).wait_recv()
        scatter_full(1, i, ox, y, i).wait_recv()
        add(ox, y, i, [(full_p, i), (full_m, i)])
        scatter_x(12 + i, ox, y, i).start()

    def far_halves(i, col, u):
        scatter_half(0, i, col, far, u).start()
        scatter_half(1, i, col, far, u).start()

    def far_later(i):
        u = FIRST + i
        scatter_x(3 + i, cx, far, u).wait_recv()
        add(cx, far, u, [(from_x, 3 + i)])
        far_halves(5 + u, cx, u)

    def side_later(i):
        u = FIRST + i
        scatter_x(i, cx, up, u).wait_recv()
        add(cx, up, u, [(from_x, i)])
        scatter_x(6 + i, cx, dn, u).wait_recv()
        add(cx, dn, u, [(from_x, 6 + i)])

    def terms(chunk):
        col, row = chunk // 4, chunk % 4
        away = (row + 4 - y) % 4
        other = (col + cx) % 2
        at = pl.ds(pl.multiple_of(chunk * ROWS, ROWS), ROWS)
        width = min(512, depth)
        for j in range(0, depth, width):
            cols = slice(j, j + width)
            low = dot_t(dqkv[at, :], weights[cols, :]).astype(bf)
            part[at, cols] = low
            moved = low.astype(f32) * xf[at, cols].astype(f32)
            gsum[:, cols] += jnp.sum(moved.reshape(ROWS // 8, 8, width), axis=0)

        @pl.when(other == 1)
        def _():
            role = (away + 3) % 4
            units(later, lambda i: scatter_x(3 * role + i, ox, row, FIRST + i).start())

        @pl.when(away == 2)
        def _():
            units(FIRST, lambda u: far_halves(5 * (1 - other) + u, col, u))

    def after_3(i):
        terms(6 + (far + i) % 2)

    def after_2(i):
        terms((1 - cx) * (4 + (far + i) % 2) + cx * (4 + far))

    def after_1(i):
        terms(2 + (far + i) % 2)

    def after_0(i):
        own = 1 - cx * (1 - (i + 2) // 4)
        k = (i - cx) * own
        d = 2 - k + 3 * (k // 2) - 2 * (k // 3)
        terms(own * (cx * 4 + (y + d) % 4) + (1 - own) * ((far + i) % 2))

        @pl.when(i == 1 + 3 * cx)
        def _():
            units(FIRST, lambda u: near(u, ox, u))

    seq = qkv.shape[0]
    after = ((after_0, 4 + cx), (after_1, 2 * cx), (after_2, 2 - cx), (after_3, 2 * (1 - cx)))
    for b in reversed(range(4)):
        start = b * BLOCK
        attention_rows(start, BLOCK, qkv, dout, table, dqkv, acc_k, acc_v, start + BLOCK == seq)
        units(after[b][1], after[b][0])

    gbuf[t] = jnp.sum(gsum[...], axis=0, keepdims=True)
    def gain_to(d):
        return rdma(gbuf.at[t], gbuf.at[t], gs.at[d], gr.at[d], (r, (t + d) % 8))

    for d in range(1, 8):
        gain_to(d).start()
    frag_step(7)

    def early_sends_ended():
        units(8, lambda i: [gather(w, i, cx, y, i).wait_send() for w in range(3)] and None)
        units(FIRST, lambda i: [gather(w, 8 + i, ox, y, i).wait_send() for w in range(2)] and None)
        units(13, lambda i: [gather(w, 13 + i, cx, y, 0, w).wait_send() for w in range(2)] and None)
        units(9, lambda i: gather(2, 8 + i, cx, y, 0).wait_send())
        for d in range(1, 8):
            gain_to(d).wait_send()
        for d in range(1, nz):
            frag_c(d).wait_send()
            frag_c_back(d).wait_send()
        frag_a().wait_send()
        frag_b().wait_send()
        frag_b_back().wait_send()
        frag_a_back().wait_send()

    def most_sends_ended():
        units(13, lambda i: [scatter_half(w, i, cx, y, 0).wait_send() for w in range(2)] and None)
        units(5 + FIRST, lambda i: [scatter_full(w, i, cx, y, 0).wait_send() for w in range(2)] and None)
        units(12, lambda i: scatter_x(i, cx, y, 0).wait_send())

    def weight_stage(j):
        @pl.when(j == 0)
        def _():
            units(3, lambda u: near(5 + u, cx, u))

        @pl.when(j == 3)
        def _():
            units(FIRST, across)

        @pl.when(j == 5)
        def _():
            units(later, far_later)
            units(FIRST - 3, lambda u: near(5 + u, cx, u), 3)

        @pl.when(j == 7)
        def _():
            units(later, side_later)

        @pl.when(j == 8)
        def _():
            units(later, lambda i: near(5 + FIRST + i, cx, FIRST + i))

        @pl.when(j == 9)
        def _():
            frag_step(8)
            for zz in range(nz):
                outer_update(zz)

        @pl.when(j == 10)
        def _():
            for d in range(1, 8):
                ref = gbuf.at[(t + 8 - d) % 8]
                rdma(ref, ref, gs.at[d], gr.at[d], (r, (t + d) % 8)).wait_recv()
            total = gbuf[0]
            for d in range(1, 8):
                total += gbuf[d]
            ggain[...] = total / gain[...]
            early_sends_ended()

        block = depth // STEPS
        at = pl.ds(pl.multiple_of(j * block, block), block)
        g = t_dot(xf[:, at], dqkv[...]).astype(bf)
        gq[at, :] = g[:, :wide_q]
        gk[at, :] = g[:, wide_q : wide_q + HEAD]
        gv[at, :] = g[:, wide_q + HEAD :]

    units(STEPS, weight_stage)
    most_sends_ended()

    def finish(u):
        @pl.when(u < FIRST)
        def _():
            scatter_x(12 + u, cx, y, u).wait_recv()

        @pl.when(u >= FIRST)
        def _():
            scatter_x(9 + u - FIRST, cx, y, u).wait_recv()

        at_x = (12 + u) * (1 - u // FIRST) + (4 + u) * (u // FIRST)
        scatter_full(0, 5 + u, cx, y, u).wait_recv()
        scatter_full(1, 5 + u, cx, y, u).wait_recv()

        def term(ref, i):
            return ref[pl.ds(pl.multiple_of(i * UNIT, UNIT), UNIT), :].astype(f32)

        mine = (cx * 4 + y) * UNITS + u
        total = (term(part, mine) + term(from_x, at_x)) + (term(full_p, 5 + u) + term(full_m, 5 + u))
        rows = pl.ds(pl.multiple_of(u * UNIT, UNIT), UNIT)
        xhat, inverse = normalise(rows, tokens)
        scaled = total * gain[...]
        mean = jnp.mean(scaled * xhat, axis=1, keepdims=True)
        gtok[rows, :] = (inverse * (scaled - xhat * mean)).astype(bf)

    units(UNITS, finish)

    units(later, lambda i: [scatter_full(w, 5 + FIRST + i, cx, y, 0).wait_send() for w in range(2)] and None)
    units(FIRST, lambda i: scatter_x(12 + i, cx, y, 0).wait_send())


def run(reps, tokens, gain, wq, wk, wv, dout, global_fragment, momentum, local_fragment):
    depth = tokens.shape[1]
    seq = dout.shape[0]
    table = rope_constants(seq)
    f32, bf = jnp.float32, jnp.bfloat16
    cols = wq.shape[1] + wk.shape[1] + wv.shape[1]
    anywhere = pl.BlockSpec(memory_space=pltpu.HBM)
    nz = reps // 4
    zcols = depth // nz
    dma = pltpu.SemaphoreType.DMA
    vm = pltpu.VMEM
    scratch = [
        vm((ROWS, depth), bf), vm((1, depth), f32), vm((seq, depth), bf), vm((depth, cols), bf),
        vm((seq, cols), bf), vm((seq, cols), bf), vm(dout.shape, bf), vm(table.shape, f32),
        vm((seq, HEAD), f32), vm((seq, HEAD), f32),
        vm((seq, depth), bf),
        vm((13 * UNIT, depth), bf), vm((13 * UNIT, depth), bf),
        vm((13 * UNIT, depth // 2), bf), vm((13 * UNIT, depth // 2), bf), vm((17 * UNIT, depth), bf),
        vm((8, 1, depth), f32), vm((8, depth), f32),
        vm((64, depth), bf), vm((32, depth), bf), vm((32, depth), f32), vm((nz, 32, zcols), f32),
        vm((32, zcols), f32), vm((16, zcols), f32), vm((nz, 32, zcols), f32), vm((nz, 32, zcols), f32),
        vm((64, depth), f32), vm((64, depth), f32),
        dma((10,)),
    ]
    scratch += [dma((n,)) for n in (26, 26, 17) * 4]
    scratch += [dma((n,)) for n in (8, 8, 4, 4, nz, nz, nz, nz)]
    operands = (tokens, gain, wq, wk, wv, dout, table, global_fragment, momentum, local_fragment)
    return pl.pallas_call(
        functools.partial(step_kernel, reps),
        out_shape=(
            jax.ShapeDtypeStruct(wq.shape, bf),
            jax.ShapeDtypeStruct(wk.shape, bf),
            jax.ShapeDtypeStruct(wv.shape, bf),
            jax.ShapeDtypeStruct((1, depth), f32),
            jax.ShapeDtypeStruct((ROWS, depth), bf),
            jax.ShapeDtypeStruct((64, depth), f32),
            jax.ShapeDtypeStruct((64, depth), f32),
        ),
        in_specs=[anywhere] * 10,
        out_specs=[pl.BlockSpec(memory_space=pltpu.VMEM)] * 7,
        scratch_shapes=scratch,
        compiler_params=pltpu.CompilerParams(
            vmem_limit_bytes=LIMIT, collective_id=0, has_side_effects=True
        ),
    )(*(pltpu.with_memory_space_constraint(a, pltpu.HBM) for a in operands))


def flush_kernel(*refs):
    count = len(refs) // 2
    sem = refs[-1]
    copies = []
    for i in range(count):
        rows = refs[i].shape[0]
        piece = rows // PIECES if rows % (16 * PIECES) == 0 else rows
        for at in range(0, rows, piece):
            part = slice(at, at + piece)
            copies.append(
                pltpu.make_async_copy(refs[i].at[part, :], refs[count + i].at[part, :], sem.at[len(copies)])
            )
    for c in copies:
        c.start()
    for c in copies:
        c.wait()


def flush(*arrays):
    return pl.pallas_call(
        flush_kernel,
        out_shape=tuple(jax.ShapeDtypeStruct(a.shape, a.dtype) for a in arrays),
        in_specs=[pl.BlockSpec(memory_space=pltpu.VMEM)] * len(arrays),
        out_specs=[pl.BlockSpec(memory_space=pl.ANY)] * len(arrays),
        scratch_shapes=[pltpu.SemaphoreType.DMA((PIECES * len(arrays),))],
        compiler_params=pltpu.CompilerParams(vmem_limit_bytes=8 * 1024 * 1024),
    )(*arrays)


def body(tokens, norm_gain, w_query, key_weight, value_weight, attention_gradient, global_fragment, momentum, local_fragment):
    replicas = lax.axis_size("rep")
    gq, gk, gv, grad_gain, grad_tokens, new_global, new_momentum = run(
        replicas, tokens[0], norm_gain, w_query[0], key_weight[0], value_weight[0],
        attention_gradient[0], global_fragment, momentum, local_fragment[0],
    )
    gq, gk, gv, grad_gain, grad_tokens, new_global, new_momentum = flush(
        gq, gk, gv, grad_gain, grad_tokens, new_global, new_momentum
    )
    return (gq[None], gk[None], gv[None], grad_gain, grad_tokens[None], new_global, new_momentum)


def solution(mesh):
    placed = (
        P("rep", "tp", None), P("rep", None), P("rep", None, "tp"), P("rep", None, "tp"), P("rep", None, "tp"),
        P("rep", None, "tp"), P("tp", None), P("tp", None), P("rep", "tp", None),
    )
    outs = (P("rep", None, "tp"), P("rep", None, "tp"), P("rep", None, "tp"), P("rep", None), P("rep", "tp", None), P("tp", None), P("tp", None))
    return jax.shard_map(body, mesh=mesh, in_specs=placed, out_specs=outs, check_vma=False)
```
